256 devices in a mesh: pop: 2 (over z), dp: 2 (over core), tensor: 64 (over y, x).
Axes of the slice: x: 8, y: 8, z: 2, core: 2. Of those that a mesh axis runs over, the one named last changes fastest.
The devices are a block of a 8x8x16 slice.
Arguments:
- tokens: bfloat16 [1024, 16384], P(('pop', 'dp'), 'tensor'), parts along dimension 0, may hold values from -6 to 6
- weight: bfloat16 [16384, 26624], P('dp', 'tensor'), may hold values from -0.046875 to 0.046875
- adapter_in: bfloat16 [8, 16384, 64], P(('pop', 'dp'), 'tensor'), parts along dimension 0, may hold values from -0.046875 to 0.046875
- adapter_out: bfloat16 [8, 64, 26624], P(('pop', 'dp'), None, 'tensor'), parts along dimension 0, may hold values from -0.375 to 0.375
- cotangent: bfloat16 [1024, 26624], P(('pop', 'dp'), 'tensor'), parts along dimension 0, may hold values from -0.59765625 to 0.59765625
- member_blocks: int32 [8], P('pop'), parts along dimension 0, may hold values from 0 to 3, as said below
- block_live: int32 [8], P(('pop', 'dp')), parts along dimension 0, may hold values from 1 to 128, as said below
Outputs:
- hidden: bfloat16 [1024, 26624], P(('pop', 'dp'), 'tensor'), parts along dimension 0
- input_gradient: bfloat16 [1024, 16384], P(('pop', 'dp'), 'tensor'), parts along dimension 0
- down_factor_gradient: float32 [8, 16384, 64], P(('pop', 'dp'), 'tensor'), parts along dimension 0
- up_factor_gradient: float32 [8, 64, 26624], P(('pop', 'dp'), None, 'tensor'), parts along dimension 0
The draws below stay inside these ranges and needn't reach their ends.
There are 2 independent parts, one for each index of `pop`. The reference program is written for one: setup_inputs(seed, part) draws one part's arguments, and reference() takes and returns one part's arrays. A program takes and returns all parts, laid end to end along the dimension named above; an argument that names none is the same for every part. Nothing has to cross between parts.
Inputs may be any that keep to these rules, and one draw needn't show every extreme that they name: `member_blocks`: the number of 128-token blocks of each member; the counts sum to 4 and the blocks come in order of member. `block_live`: the live tokens stand at the start of each block; every block but the last one of its member is full.
All inputs are finite; a program needn't handle non-finite values.
Results may differ from the reference program's by a relative error of at most 0.003.
Values may be sent and summed in bfloat16 or wider, within the bound.
No kernel may reach another device: no remote copies, remote signals or barrier semaphores. Data moves between devices by JAX's collectives and lax.ppermute only.
A program may use at most 128 MiB of HBM per device.

```python
import jax
import jax.numpy as jnp
from jax import lax

D = 16384
FFW = 26624
MEMBERS = 4
RANK = 64
BLOCK = 128
TOKENS = 512
NBLK = 4


def member_layout(key):
    salted = jax.random.fold_in(key, 31)
    first_key, second_key, third_key = jax.random.split(salted, 3)
    biggest = NBLK // 2 + 1
    leader = jax.random.randint(third_key, (), 0, MEMBERS).astype(jnp.int32)
    others = jax.random.randint(first_key, (NBLK - biggest,), 0, MEMBERS - 1).astype(jnp.int32)
    others = (others + (others >= leader).astype(jnp.int32)).astype(jnp.int32)
    leading = jnp.zeros((biggest,), dtype=jnp.int32) + leader
    members = jnp.sort(jnp.concatenate([leading, others])).astype(jnp.int32)
    return (members, second_key)


def draw_member_blocks(key, part):
    members, second_key = member_layout(key)
    hits = (members[:, None] == jnp.arange(MEMBERS, dtype=jnp.int32)[None, :]).astype(jnp.int32)
    return jnp.sum(hits, axis=0).astype(jnp.int32)


def draw_block_live(key, part):
    members, second_key = member_layout(key)
    closing = jnp.concatenate([members[1:] != members[:-1], jnp.ones((1,), dtype=jnp.bool_)])
    partial_fill = jax.random.randint(second_key, (NBLK,), 1, BLOCK + 1)
    return jnp.where(closing, partial_fill, BLOCK).astype(jnp.int32)


def level_of(own_key, extent, cuts, low, largest):
    def one(position, shards_of):
        heights = jax.random.uniform(jax.random.fold_in(jax.random.fold_in(own_key, 6), position), (shards_of,), jnp.float32, low / len(cuts), largest / len(cuts))
        return jnp.repeat(jnp.exp(heights), extent[position] // shards_of).reshape((-1,) + (1,) * (len(extent) - position - 1))

    factor_of = one(*cuts[0])
    for cut in cuts[1:]:
        factor_of = factor_of * one(*cut)
    return factor_of


def gaussian(own_key, extent, deviation, bound, pieces=(), held_as=jnp.bfloat16):
    array = jax.random.normal(own_key, extent, jnp.float32) * deviation
    if len(pieces) > 0:
        array = level_of(own_key, extent, pieces, -0.22, 0.18) * array
    return jnp.clip(array, min=-bound, max=bound).astype(held_as)


def setup_inputs(seed: int = 0, part: int = 0) -> dict:
    streams_of = jax.random.split(jax.random.key(seed), 8)
    part_splits = jax.random.split(jax.random.fold_in(streams_of[7], part), 8)
    tokens = gaussian(part_splits[0], (TOKENS, D), 1.0, 6.0, ((0, 2), (1, 64)))
    weight = gaussian(streams_of[1], (D, FFW), D ** -0.5, 0.046875, ((0, 2), (1, 64)))
    adapter_in = gaussian(part_splits[2], (MEMBERS, D, RANK), D ** -0.5, 0.046875, ((0, 2), (1, 64)))
    adapter_out = gaussian(part_splits[3], (MEMBERS, RANK, FFW), (4 * RANK) ** -0.5, 0.375, ((0, 2), (2, 64)))
    cotangent = gaussian(part_splits[4], (TOKENS, FFW), 0.1, 0.59765625, ((0, 2), (1, 64)))
    member_blocks = draw_member_blocks(jax.random.fold_in(jax.random.fold_in(streams_of[7], part), 71), part)
    block_live = draw_block_live(jax.random.fold_in(jax.random.fold_in(streams_of[7], part), 71), part)
    return {"tokens": tokens, "weight": weight, "adapter_in": adapter_in, "adapter_out": adapter_out, "cotangent": cotangent, "member_blocks": member_blocks, "block_live": block_live}


adapter_scale = 0.5


def reference(tokens, weight, adapter_in, adapter_out, cotangent, member_blocks, block_live):
    ends = jnp.cumsum(member_blocks).astype(jnp.int32)
    blocks = jnp.arange(NBLK, dtype=jnp.int32)
    members = jnp.sum((ends[None, :] <= blocks[:, None]).astype(jnp.int32), axis=1).astype(jnp.int32)
    member_lookup = (members[:, None] == jnp.arange(MEMBERS, dtype=jnp.int32)[None, :]).astype(jnp.float32)
    offsets = jnp.arange(BLOCK, dtype=jnp.int32)
    active_member_mask = (offsets[None, :] < block_live[:, None]).astype(jnp.bfloat16).reshape(TOKENS, 1)
    chosen_in = jnp.take(adapter_in, members, axis=0).astype(jnp.float32)
    chosen_out = jnp.take(adapter_out, members, axis=0).astype(jnp.float32)
    token_blocks = tokens.reshape(NBLK, BLOCK, D).astype(jnp.float32)
    low_in = jnp.einsum("btk,bkr->btr", token_blocks, chosen_in).astype(jnp.bfloat16)
    frozen_projection = jnp.dot(tokens, weight, preferred_element_type=jnp.float32)
    raised_hidden = jnp.einsum("btr,brf->btf", low_in.astype(jnp.float32), chosen_out).reshape(TOKENS, FFW)
    hidden = (active_member_mask.astype(jnp.float32) * (frozen_projection + adapter_scale * raised_hidden)).astype(jnp.bfloat16)
    masked = cotangent * active_member_mask
    grad_blocks = masked.reshape(NBLK, BLOCK, FFW).astype(jnp.float32)
    low_back = jnp.einsum("btf,brf->btr", grad_blocks, chosen_out).astype(jnp.bfloat16)
    projected_output = lax.dot_general(masked, weight, (((1,), (1,)), ((), ())), preferred_element_type=jnp.float32)
    reduced_hidden = jnp.einsum("btr,bkr->btk", low_back.astype(jnp.float32), chosen_in).reshape(TOKENS, D)
    input_gradient = (projected_output + adapter_scale * reduced_hidden).astype(jnp.bfloat16)
    down_outer_product = jnp.einsum("btk,btr->bkr", token_blocks, low_back.astype(jnp.float32))
    up_outer_product = jnp.einsum("btr,btf->brf", low_in.astype(jnp.float32), grad_blocks)
    down_factor_gradient = adapter_scale * jnp.einsum("gw,gsd->wsd", member_lookup, down_outer_product, precision=lax.Precision.HIGHEST)
    up_factor_gradient = adapter_scale * jnp.einsum("jg,juy->guy", member_lookup, up_outer_product, precision=lax.Precision.HIGHEST)
    return hidden, input_gradient, down_factor_gradient, up_factor_gradient
```

```python
import functools
import math

import jax
import jax.numpy as jnp
from jax import lax
from jax.experimental import pallas as pl
from jax.experimental.pallas import tpu as pltpu
from jax.sharding import Mesh
from jax.sharding import PartitionSpec as P

MEMBERS = 4
BLOCK = 128
TENSOR = ("ty", "tx")
GROUP = ("dp", "ty", "tx")
EXTRA = 16
TOP = 32767.0


adapter_scale = 0.5


def ring_pairs(side, step, bulk):
    pairs = []
    for c in range(2):
        for y in range(side):
            for x in range(side):
                along_y = (c == 0) == bulk
                to_y = (y + step) % side if along_y else y
                to_x = x if along_y else (x + step) % side
                pairs.append(
                    ((c * side + y) * side + x, (c * side + to_y) * side + to_x)
                )
    return pairs


def send(x, side, step, bulk):
    return lax.ppermute(x, GROUP, ring_pairs(side, step, bulk))


def swap(x):
    return lax.ppermute(x, "dp", [(0, 1), (1, 0)])


def start_weight(pos, own, other, buf, sem, slot, side, d, i):
    c, p, q = pos[0], pos[1], pos[2]
    chunk = lax.rem(p + (d + side), side)
    piece = lax.rem(q + (side - i), side)
    t = jnp.where(c == 0, side * chunk + piece, side * piece + chunk)
    here = own.shape[0]
    half = (t >= here).astype(jnp.int32)
    row = t - half * here

    @pl.when(half == c)
    def _():
        pltpu.make_async_copy(own.at[row], buf.at[slot], sem.at[slot]).start()

    @pl.when(half != c)
    def _():
        pltpu.make_async_copy(other.at[row], buf.at[slot], sem.at[slot]).start()


def wait_weight(own, buf, sem, slot):
    pltpu.make_async_copy(own.at[0], buf.at[slot], sem.at[slot]).wait()


def coded(acc):
    top = jnp.maximum(jnp.max(jnp.abs(acc), axis=0, keepdims=True), 1e-30)
    e = jnp.ceil(jnp.log2(top))
    q = jnp.round(acc * (jnp.exp2(-e) * TOP))
    q = jnp.clip(q, -TOP, TOP)
    return q.astype(jnp.int32).astype(jnp.int16), e


def scales(rows):
    return jnp.exp2(rows.astype(jnp.int32).astype(jnp.float32)) * (1.0 / TOP)


def reduce_kernel(pos, m, own, other, *refs, side, d, pieces, arrived, last):
    refs = list(refs)
    recv = [refs.pop(0) for _ in arrived]
    if last:
        mine = refs.pop(0)
        outs = [refs.pop(0) for _ in pieces[1:]]
    else:
        out = refs.pop(0)
    wbuf, sem, es, *sin = refs
    n = own.shape[1]
    for k, i in enumerate(pieces):
        start_weight(pos, own, other, wbuf, sem, k, side, d, i)
    for r, s, held in zip(recv, sin, arrived):
        s[...] = scales(r[len(held) * n :, :])
    es[...] = jnp.zeros_like(es)
    for k, i in enumerate(pieces):
        wait_weight(own, wbuf, sem, k)
        acc = lax.dot_general(
            m[...], wbuf[k], (((1,), (1,)), ((), ())), preferred_element_type=jnp.float32
        )
        for r, s, held in zip(recv, sin, arrived):
            if i in held:
                h = held.index(i)
                part = r[h * n : (h + 1) * n, :].astype(jnp.int32).astype(jnp.float32)
                acc = acc + part * s[h : h + 1, :]
        if last and k == 0:
            mine[...] = acc
            continue
        q, e = coded(acc)
        if last:
            outs[k - 1][:n, :] = q
            outs[k - 1][n:, :] = (
                jnp.broadcast_to(e, (EXTRA, n)).astype(jnp.int32).astype(jnp.int16)
            )
        else:
            out[k * n : (k + 1) * n, :] = q
            es[k : k + 1, :] = e
    if not last:
        out[len(pieces) * n :, :] = es[...].astype(jnp.int32).astype(jnp.int16)


def reduce_step(pos, masked, own, other, recv, arrived, side, d, pieces, last=False):
    tokens, n, width = masked.shape[0], own.shape[1], own.shape[2]
    if last:
        out_shape = [jax.ShapeDtypeStruct((tokens, n), jnp.float32)] + [
            jax.ShapeDtypeStruct((tokens + EXTRA, n), jnp.int16) for _ in pieces[1:]
        ]
    else:
        out_shape = jax.ShapeDtypeStruct((len(pieces) * tokens + EXTRA, n), jnp.int16)
    vmem = pl.BlockSpec(memory_space=pltpu.VMEM)
    hbm = pl.BlockSpec(memory_space=pl.ANY)
    return pl.pallas_call(
        functools.partial(
            reduce_kernel, side=side, d=d, pieces=pieces, arrived=arrived, last=last
        ),
        out_shape=out_shape,
        in_specs=[pl.BlockSpec(memory_space=pltpu.SMEM), vmem, hbm, hbm]
        + [vmem] * len(recv),
        out_specs=[vmem] * len(pieces) if last else vmem,
        scratch_shapes=[
            pltpu.VMEM((len(pieces), n, width), own.dtype),
            pltpu.SemaphoreType.DMA((len(pieces),)),
            pltpu.VMEM((EXTRA, n), jnp.float32),
        ]
        + [pltpu.VMEM((EXTRA, n), jnp.float32) for _ in recv],
        cost_estimate=pl.CostEstimate(
            flops=2 * tokens * n * width * len(pieces),
            bytes_accessed=len(pieces) * n * (width + tokens * 2) * 2,
            transcendentals=0,
        ),
    )(pos, masked, own, other, *recv)


def gather_kernel(pos, acc, own, other, *refs, side, held, last):
    refs = list(refs)
    chunks = [refs.pop(0) for _ in held]
    if last:
        extra, live = refs.pop(0), refs.pop(0)
    out, xbuf, wbuf, xsem, wsem = refs
    n = own.shape[1]
    slot = 0
    for x, (d, pieces) in zip(chunks, held):
        for h, i in enumerate(pieces):
            start_weight(pos, own, other, wbuf, wsem, slot, side, d, i)
            pltpu.make_async_copy(
                x.at[pl.ds(h * n, n)], xbuf.at[slot], xsem.at[slot]
            ).start()
            slot += 1
    total = acc[...]
    slot = 0
    for x, (d, pieces) in zip(chunks, held):
        for h, i in enumerate(pieces):
            wait_weight(own, wbuf, wsem, slot)
            pltpu.make_async_copy(
                x.at[pl.ds(h * n, n)], xbuf.at[slot], xsem.at[slot]
            ).wait()
            total = total + jnp.dot(
                xbuf[slot], wbuf[slot], preferred_element_type=jnp.float32
            )
            slot += 1
    if last:
        total = live[...] * (total + adapter_scale * extra[...])
    out[...] = total.astype(out.dtype)


def gather_step(pos, acc, own, other, chunks, held, side, extra=()):
    n, width = own.shape[1], own.shape[2]
    tokens = acc.shape[0]
    count = sum(len(pieces) for _, pieces in held)
    vmem = pl.BlockSpec(memory_space=pltpu.VMEM)
    hbm = pl.BlockSpec(memory_space=pl.ANY)
    last = len(extra) > 0
    return pl.pallas_call(
        functools.partial(gather_kernel, side=side, held=held, last=last),
        out_shape=jax.ShapeDtypeStruct(acc.shape, jnp.bfloat16 if last else jnp.float32),
        in_specs=[pl.BlockSpec(memory_space=pltpu.SMEM), vmem, hbm, hbm]
        + [hbm] * len(chunks)
        + [vmem] * len(extra),
        out_specs=vmem,
        scratch_shapes=[
            pltpu.VMEM((count, tokens, n), jnp.bfloat16),
            pltpu.VMEM((count, n, width), own.dtype),
            pltpu.SemaphoreType.DMA((count,)),
            pltpu.SemaphoreType.DMA((count,)),
        ],
        cost_estimate=pl.CostEstimate(
            flops=2 * tokens * n * width * count,
            bytes_accessed=count * n * (width + tokens) * 2,
            transcendentals=0,
        ),
    )(pos, acc, own, other, *chunks, *extra)


def finish_kernel(mine, extra, *refs):
    *parts, out = refs
    n = mine.shape[0]
    total = mine[...] + adapter_scale * extra[...]
    for r in parts:
        s = scales(r[n:, :])[0:1, :]
        total = total + r[:n, :].astype(jnp.int32).astype(jnp.float32) * s
    out[...] = total.astype(out.dtype)


def finish(mine, extra, parts):
    return pl.pallas_call(
        finish_kernel,
        out_shape=jax.ShapeDtypeStruct(mine.shape, jnp.bfloat16),
    )(mine, extra, *parts)


def block_members(member_blocks, first, count):
    ends = jnp.cumsum(member_blocks)
    blocks = first + jnp.arange(count, dtype=jnp.int32)
    return jnp.sum((ends[None, :] <= blocks[:, None]).astype(jnp.int32), axis=1)


def both_halves(x, c):
    other = swap(x)
    first = jnp.where(c == 0, x, other)
    second = jnp.where(c == 0, other, x)
    return jnp.concatenate([first, second], axis=0)


def sum_over_group(x, count):
    rows = x.shape[0] // count
    pieces = lax.all_to_all(
        x.reshape(count, rows, x.shape[1]), TENSOR, split_axis=0, concat_axis=0, tiled=True
    )
    part = pieces.sum(axis=0)
    every = jnp.broadcast_to(part[None], (count, *part.shape))
    every = lax.all_to_all(every, TENSOR, split_axis=0, concat_axis=0, tiled=True)
    return every.reshape(x.shape)


def local(tokens, weight, adapter_in, adapter_out, cotangent, member_blocks, block_live, *, side):
    token_rows, width_local = tokens.shape
    hidden_local = weight.shape[1]
    blocks_here = token_rows // BLOCK
    c = lax.axis_index("dp").astype(jnp.int32)
    y = lax.axis_index("ty").astype(jnp.int32)
    x = lax.axis_index("tx").astype(jnp.int32)
    pos = jnp.stack([c, jnp.where(c == 0, y, x), jnp.where(c == 0, x, y)])
    far = side // 2
    every = tuple(range(side))
    low_half, high_half = every[:far], every[far:]

    own = weight.reshape(-1, width_local, hidden_local)
    other = swap(weight).reshape(own.shape)

    shifts = [s if s <= far else s - side for s in range(side)]
    pieces = [tokens] + [send(tokens, side, s, False) for s in shifts[1:]]
    home = jnp.concatenate(pieces, axis=0)

    members = block_members(member_blocks, c * blocks_here, blocks_here)
    offsets = jnp.arange(BLOCK, dtype=jnp.int32)
    live = (offsets[None, :] < block_live[:, None]).astype(jnp.bfloat16).reshape(token_rows, 1)
    masked = cotangent * live

    down_all = both_halves(adapter_in, c)
    up_all = both_halves(adapter_out, c)
    chosen_in = jnp.take(down_all, members, axis=0)
    chosen_out = jnp.take(up_all, members, axis=0)
    token_blocks = tokens.reshape(blocks_here, BLOCK, width_local)
    grad_blocks = masked.reshape(blocks_here, BLOCK, hidden_local)
    part_in = jnp.einsum(
        "btk,bkr->btr", token_blocks, chosen_in, preferred_element_type=jnp.float32
    )
    part_back = jnp.einsum(
        "btf,brf->btr", grad_blocks, chosen_out, preferred_element_type=jnp.float32
    )
    rank = part_in.shape[-1]
    both = jnp.concatenate([part_in, part_back], axis=-1).reshape(token_rows, 2 * rank)
    sums = sum_over_group(both, side * side).astype(jnp.bfloat16)
    low_in = sums[:, :rank].reshape(blocks_here, BLOCK, rank)
    low_back = sums[:, rank:].reshape(blocks_here, BLOCK, rank)

    step = functools.partial(reduce_step, pos, masked, own, other, side=side)
    up = step([], (), d=far, pieces=low_half)
    down = step([], (), d=-far, pieces=high_half)
    ahead, behind = home, home
    total = jnp.zeros((token_rows, hidden_local), jnp.float32)
    total = gather_step(pos, total, own, other, [home], ((0, every),), side)
    held_up, held_down = low_half, high_half
    for k in range(1, far + 1):
        up = send(up, side, 1, True)
        down = send(down, side, -1, True)
        if k < far:
            ahead = send(ahead, side, 1, True)
            behind = send(behind, side, -1, True)
        else:
            ahead = send(ahead[: ahead.shape[0] // 2], side, 1, True)
            behind = send(behind[behind.shape[0] // 2 :], side, -1, True)
        if k < far:
            up = step([up], (held_up,), d=far - k, pieces=every)
            down = step([down], (held_down,), d=k - far, pieces=every)
            held_up = held_down = every
            total = gather_step(
                pos, total, own, other, [ahead, behind], ((-k, every), (k, every)), side
            )
    mine, *leaving = step([up, down], (held_up, held_down), d=0, pieces=every, last=True)
    arrived = [send(a, side, -s, False) for a, s in zip(leaving, shifts[1:])]

    raised = jnp.einsum("btr,brf->btf", low_in, chosen_out, preferred_element_type=jnp.float32)
    hidden = gather_step(
        pos,
        total,
        own,
        other,
        [ahead, behind],
        ((-far, low_half), (far, high_half)),
        side,
        extra=(raised.reshape(token_rows, hidden_local), live.astype(jnp.float32)),
    )
    reduced = jnp.einsum("btr,bkr->btk", low_back, chosen_in, preferred_element_type=jnp.float32)
    input_gradient = finish(mine, reduced.reshape(token_rows, width_local), arrived)

    down_outer = jnp.einsum(
        "btk,btr->bkr", token_blocks, low_back, preferred_element_type=jnp.float32
    )
    up_outer = jnp.einsum("btr,btf->brf", low_in, grad_blocks, preferred_element_type=jnp.float32)

    def of_members(outer, first):
        owners = first + jnp.arange(MEMBERS // 2, dtype=jnp.int32)
        picked = (owners[:, None] == members[None, :])[:, :, None, None]
        return adapter_scale * jnp.where(picked, outer[None], 0.0).sum(axis=1)

    held_here = MEMBERS // 2
    down_grad = of_members(down_outer, c * held_here) + swap(
        of_members(down_outer, (1 - c) * held_here)
    )
    up_grad = of_members(up_outer, c * held_here) + swap(
        of_members(up_outer, (1 - c) * held_here)
    )
    return (hidden, input_gradient, down_grad, up_grad)


def solution(mesh):
    side = math.isqrt(mesh.shape["tensor"])
    assert side * side == mesh.shape["tensor"] and mesh.shape["dp"] == 2
    finer = Mesh(
        mesh.devices.reshape(mesh.shape["pop"], mesh.shape["dp"], side, side),
        ("pop", "dp", "ty", "tx"),
    )
    placed = (
        P(("pop", "dp"), TENSOR),
        P("dp", TENSOR),
        P(("pop", "dp"), TENSOR, None),
        P(("pop", "dp"), None, TENSOR),
        P(("pop", "dp"), TENSOR),
        P("pop"),
        P(("pop", "dp")),
    )
    return jax.shard_map(
        functools.partial(local, side=side),
        mesh=finer,
        in_specs=placed,
        out_specs=(
            P(("pop", "dp"), TENSOR),
            P(("pop", "dp"), TENSOR),
            P(("pop", "dp"), TENSOR, None),
            P(("pop", "dp"), None, TENSOR),
        ),
        check_vma=False,
    )
```

```python
import functools
import math

import jax
import jax.numpy as jnp
from jax import lax
from jax.experimental import pallas as pl
from jax.experimental.pallas import tpu as pltpu
from jax.sharding import Mesh
from jax.sharding import PartitionSpec as P

MEMBERS = 4
BLOCK = 128
TENSOR = ("ty", "tx")
GROUP = ("dp", "ty", "tx")
EXTRA = 16
TOP = 32767.0


adapter_scale = 0.5


def ring_pairs(side, step, bulk):
    pairs = []
    for c in range(2):
        for y in range(side):
            for x in range(side):
                along_y = (c == 0) == bulk
                to_y = (y + step) % side if along_y else y
                to_x = x if along_y else (x + step) % side
                pairs.append(
                    ((c * side + y) * side + x, (c * side + to_y) * side + to_x)
                )
    return pairs


def send(x, side, step, bulk):
    return lax.ppermute(x, GROUP, ring_pairs(side, step, bulk))


def swap(x):
    return lax.ppermute(x, "dp", [(0, 1), (1, 0)])


def vmem(x):
    return pltpu.with_memory_space_constraint(x, pltpu.VMEM)


SCALARS = pl.BlockSpec(memory_space=pltpu.SMEM)
HBM = pl.BlockSpec(memory_space=pltpu.HBM)
ALL_VMEM = pl.BlockSpec(memory_space=pltpu.VMEM)
PARAMS = pltpu.CompilerParams(vmem_limit_bytes=10 << 20)


def start_weight(pos, own, other, buf, sem, slot, side, d, i):
    n = buf.shape[2]
    c, p, q = pos[0], pos[1], pos[2]
    chunk = lax.rem(p + (d + side), side)
    piece = lax.rem(q + (side - i), side)
    t = jnp.where(c == 0, side * chunk + piece, side * piece + chunk)
    here = own.shape[1] // n
    half = (t >= here).astype(jnp.int32)
    at = pl.ds(pl.multiple_of((t - half * here) * n, n), n)

    @pl.when(half == c)
    def _():
        pltpu.make_async_copy(own.at[:, at], buf.at[slot], sem.at[slot]).start()

    @pl.when(half != c)
    def _():
        pltpu.make_async_copy(other.at[:, at], buf.at[slot], sem.at[slot]).start()


def wait_weight(own, buf, sem, slot):
    n = buf.shape[2]
    pltpu.make_async_copy(own.at[:, pl.ds(0, n)], buf.at[slot], sem.at[slot]).wait()


def coded(acc):
    top = jnp.maximum(jnp.max(jnp.abs(acc), axis=0, keepdims=True), 1e-30)
    e = jnp.ceil(jnp.log2(top))
    q = jnp.round(acc * (jnp.exp2(-e) * TOP))
    q = jnp.clip(q, -TOP, TOP)
    return q.astype(jnp.int32).astype(jnp.int16), e


def scales(rows):
    return jnp.exp2(rows.astype(jnp.int32).astype(jnp.float32)) * (1.0 / TOP)


def reduce_kernel(pos, m, own, other, *refs, side, d, first, count, arrived, last):
    refs = list(refs)
    recv = [refs.pop(0) for _ in arrived]
    if last:
        mine = refs.pop(0)
        outs = [refs.pop(0) for _ in range(count - 1)]
    else:
        out = refs.pop(0)
    wbuf, sem, es, *sin = refs
    n = m.shape[0]

    def begin(k, _):
        start_weight(pos, own, other, wbuf, sem, k, side, d, first + k)
        return 0

    lax.fori_loop(0, count, begin, 0)
    for r, s, (_, held) in zip(recv, sin, arrived):
        s[...] = scales(r[held * n :, :])

    def piece(k, added):
        wait_weight(own, wbuf, sem, k)
        acc = jnp.dot(m[...], wbuf[k], preferred_element_type=jnp.float32)
        for r, s, (start, _) in added:
            h = k + (first - start)
            at = pl.ds(pl.multiple_of(h * n, n), n)
            acc = acc + r[at, :].astype(jnp.int32).astype(jnp.float32) * s[pl.ds(h, 1), :]
        return acc

    parts = list(zip(recv, sin, arrived))
    if last:
        mine[...] = piece(0, parts)
        for k in range(1, count):
            q, e = coded(piece(k, parts))
            outs[k - 1][:n, :] = q
            outs[k - 1][n:, :] = (
                jnp.broadcast_to(e, (EXTRA, n)).astype(jnp.int32).astype(jnp.int16)
            )
        return

    es[...] = jnp.zeros_like(es)

    def body(k, _, added):
        q, e = coded(piece(k, added))
        out[pl.ds(pl.multiple_of(k * n, n), n), :] = q
        es[pl.ds(k, 1), :] = e
        return 0

    cuts = sorted({0, count, *(v for a, h in arrived for v in (a - first, a - first + h))})
    for lo, hi in zip(cuts, cuts[1:]):
        added = [t for t in parts if t[2][0] - first <= lo and hi <= t[2][0] - first + t[2][1]]
        lax.fori_loop(lo, hi, functools.partial(body, added=added), 0, unroll=2)
    out[count * n :, :] = es[...].astype(jnp.int32).astype(jnp.int16)


def reduce_step(pos, masked, own, other, recv, arrived, side, d, first, count, last=False):
    tokens, width = masked.shape
    n = tokens
    if last:
        out_shape = [pltpu.VMEM((tokens, n), jnp.float32)] + [
            pltpu.VMEM((tokens + EXTRA, n), jnp.int16) for _ in range(count - 1)
        ]
    else:
        out_shape = pltpu.VMEM((count * tokens + EXTRA, n), jnp.int16)
    return pl.pallas_call(
        functools.partial(
            reduce_kernel,
            side=side,
            d=d,
            first=first,
            count=count,
            arrived=arrived,
            last=last,
        ),
        out_shape=out_shape,
        in_specs=[SCALARS, ALL_VMEM, HBM, HBM] + [ALL_VMEM] * len(recv),
        out_specs=[ALL_VMEM] * count if last else ALL_VMEM,
        scratch_shapes=[
            pltpu.VMEM((count, width, n), own.dtype),
            pltpu.SemaphoreType.DMA((count,)),
        ]
        + [pltpu.VMEM((EXTRA, n), jnp.float32) for _ in range(1 + len(recv))],
        compiler_params=PARAMS,
        cost_estimate=pl.CostEstimate(
            flops=2 * tokens * n * width * count,
            bytes_accessed=count * n * (width + tokens * 2) * 2,
            transcendentals=0,
        ),
    )(pos, vmem(masked), own, other, *map(vmem, recv))


def gather_kernel(pos, acc, own, other, *refs, side, held, last):
    refs = list(refs)
    chunks = [refs.pop(0) for _ in held]
    if last:
        extra, live = refs.pop(0), refs.pop(0)
    out, total, wbuf, sem = refs
    n = acc.shape[1]
    slots = []
    for d, first, count in held:
        at = slots[-1][1] if slots else 0
        slots.append((at, at + count))

        def begin(k, _, d=d, first=first, at=at):
            start_weight(pos, own, other, wbuf, sem, at + k, side, d, first + k)
            return 0

        lax.fori_loop(0, count, begin, 0)
    total[...] = acc[...]
    for x, (at, end) in zip(chunks, slots):

        def body(k, _, x=x, at=at):
            wait_weight(own, wbuf, sem, at + k)
            rows = x[pl.ds(pl.multiple_of(k * n, n), n), :]
            total[...] += lax.dot_general(
                wbuf[at + k],
                rows,
                (((1,), (1,)), ((), ())),
                preferred_element_type=jnp.float32,
            )
            return 0

        lax.fori_loop(0, end - at, body, 0, unroll=2)
    result = total[...]
    if last:
        result = live[...] * (result + adapter_scale * extra[...])
    out[...] = result.astype(out.dtype)


def gather_step(pos, acc, own, other, chunks, held, side, extra=()):
    width, tokens = acc.shape
    count = sum(c for _, _, c in held)
    last = len(extra) > 0
    return pl.pallas_call(
        functools.partial(gather_kernel, side=side, held=held, last=last),
        out_shape=pltpu.VMEM(acc.shape, jnp.bfloat16 if last else jnp.float32),
        in_specs=[SCALARS, ALL_VMEM, HBM, HBM] + [ALL_VMEM] * (len(chunks) + len(extra)),
        out_specs=ALL_VMEM,
        scratch_shapes=[
            pltpu.VMEM(acc.shape, jnp.float32),
            pltpu.VMEM((count, width, tokens), own.dtype),
            pltpu.SemaphoreType.DMA((count,)),
        ],
        compiler_params=PARAMS,
        cost_estimate=pl.CostEstimate(
            flops=2 * tokens * tokens * width * count,
            bytes_accessed=count * tokens * (width + tokens) * 2,
            transcendentals=0,
        ),
    )(pos, vmem(acc), own, other, *map(vmem, chunks), *map(vmem, extra))


def finish_kernel(mine, extra, *refs):
    *parts, out = refs
    n = mine.shape[0]
    total = mine[...] + adapter_scale * extra[...]
    for r in parts:
        s = scales(r[n:, :])[0:1, :]
        total = total + r[:n, :].astype(jnp.int32).astype(jnp.float32) * s
    out[...] = total.astype(out.dtype)


def finish(mine, extra, parts):
    return pl.pallas_call(
        finish_kernel,
        out_shape=jax.ShapeDtypeStruct(mine.shape, jnp.bfloat16),
        in_specs=[ALL_VMEM] * (2 + len(parts)),
        out_specs=ALL_VMEM,
        compiler_params=PARAMS,
    )(*map(vmem, (mine, extra, *parts)))


def block_members(member_blocks, first, count):
    ends = jnp.cumsum(member_blocks)
    blocks = first + jnp.arange(count, dtype=jnp.int32)
    return jnp.sum((ends[None, :] <= blocks[:, None]).astype(jnp.int32), axis=1)


def both_halves(x, c):
    other = swap(x)
    first = jnp.where(c == 0, x, other)
    second = jnp.where(c == 0, other, x)
    return jnp.concatenate([first, second], axis=0)


def sum_over_group(x, count):
    rows = x.shape[0] // count
    pieces = lax.all_to_all(
        x.reshape(count, rows, x.shape[1]), TENSOR, split_axis=0, concat_axis=0, tiled=True
    )
    part = pieces.sum(axis=0)
    every = jnp.broadcast_to(part[None], (count, *part.shape))
    every = lax.all_to_all(every, TENSOR, split_axis=0, concat_axis=0, tiled=True)
    return every.reshape(x.shape)


def local(tokens, weight, adapter_in, adapter_out, cotangent, member_blocks, block_live, *, side):
    token_rows, width_local = tokens.shape
    hidden_local = weight.shape[1]
    blocks_here = token_rows // BLOCK
    c = lax.axis_index("dp").astype(jnp.int32)
    y = lax.axis_index("ty").astype(jnp.int32)
    x = lax.axis_index("tx").astype(jnp.int32)
    pos = jnp.stack([c, jnp.where(c == 0, y, x), jnp.where(c == 0, x, y)])
    far = side // 2

    own = weight.T
    other = swap(own)
    own, other = (pltpu.with_memory_space_constraint(w, pltpu.HBM) for w in (own, other))

    shifts = [s if s <= far else s - side for s in range(side)]
    pieces = [tokens] + [send(tokens, side, s, False) for s in shifts[1:]]
    home = jnp.concatenate(pieces, axis=0)

    members = block_members(member_blocks, c * blocks_here, blocks_here)
    offsets = jnp.arange(BLOCK, dtype=jnp.int32)
    live = (offsets[None, :] < block_live[:, None]).astype(jnp.bfloat16).reshape(token_rows, 1)
    masked = cotangent * live

    down_all = both_halves(adapter_in, c)
    up_all = both_halves(adapter_out, c)
    chosen_in = jnp.take(down_all, members, axis=0)
    chosen_out = jnp.take(up_all, members, axis=0)
    token_blocks = tokens.reshape(blocks_here, BLOCK, width_local)
    grad_blocks = masked.reshape(blocks_here, BLOCK, hidden_local)
    part_in = jnp.einsum(
        "btk,bkr->btr", token_blocks, chosen_in, preferred_element_type=jnp.float32
    )
    part_back = jnp.einsum(
        "btf,brf->btr", grad_blocks, chosen_out, preferred_element_type=jnp.float32
    )
    rank = part_in.shape[-1]
    both = jnp.concatenate([part_in, part_back], axis=-1).reshape(token_rows, 2 * rank)
    sums = sum_over_group(both, side * side).astype(jnp.bfloat16)
    low_in = sums[:, :rank].reshape(blocks_here, BLOCK, rank)
    low_back = sums[:, rank:].reshape(blocks_here, BLOCK, rank)

    step = functools.partial(reduce_step, pos, masked, own, other, side=side)
    up = step([], (), d=far, first=0, count=far)
    down = step([], (), d=-far, first=far, count=far)
    ahead, behind = home, home
    total = jnp.zeros((hidden_local, token_rows), jnp.float32)
    total = gather_step(pos, total, own, other, [home], ((0, 0, side),), side)
    held_up, held_down = (0, far), (far, far)
    for k in range(1, far + 1):
        up = send(up, side, 1, True)
        down = send(down, side, -1, True)
        if k < far:
            ahead = send(ahead, side, 1, True)
            behind = send(behind, side, -1, True)
            up = step([up], (held_up,), d=far - k, first=0, count=side)
            down = step([down], (held_down,), d=k - far, first=0, count=side)
            held_up = held_down = (0, side)
            total = gather_step(
                pos,
                total,
                own,
                other,
                [ahead, behind],
                ((-k, 0, side), (k, 0, side)),
                side,
            )
        else:
            ahead = send(ahead[: ahead.shape[0] // 2], side, 1, True)
            behind = send(behind[behind.shape[0] // 2 :], side, -1, True)
    mine, *leaving = step(
        [up, down], (held_up, held_down), d=0, first=0, count=side, last=True
    )
    arrived = [send(a, side, -s, False) for a, s in zip(leaving, shifts[1:])]

    raised = jnp.einsum("btr,brf->fbt", low_in, chosen_out, preferred_element_type=jnp.float32)
    hidden = gather_step(
        pos,
        total,
        own,
        other,
        [ahead, behind],
        ((-far, 0, far), (far, far, far)),
        side,
        extra=(raised.reshape(hidden_local, token_rows), live.astype(jnp.float32).reshape(1, token_rows)),
    ).T
    reduced = jnp.einsum("btr,bkr->btk", low_back, chosen_in, preferred_element_type=jnp.float32)
    input_gradient = finish(mine, reduced.reshape(token_rows, width_local), arrived)

    down_outer = jnp.einsum(
        "btk,btr->bkr", token_blocks, low_back, preferred_element_type=jnp.float32
    )
    up_outer = jnp.einsum("btr,btf->brf", low_in, grad_blocks, preferred_element_type=jnp.float32)

    def of_members(outer, first):
        owners = first + jnp.arange(MEMBERS // 2, dtype=jnp.int32)
        picked = (owners[:, None] == members[None, :])[:, :, None, None]
        return adapter_scale * jnp.where(picked, outer[None], 0.0).sum(axis=1)

    held_here = MEMBERS // 2
    down_grad = of_members(down_outer, c * held_here) + swap(
        of_members(down_outer, (1 - c) * held_here)
    )
    up_grad = of_members(up_outer, c * held_here) + swap(
        of_members(up_outer, (1 - c) * held_here)
    )
    return (hidden, input_gradient, down_grad, up_grad)


def solution(mesh):
    side = math.isqrt(mesh.shape["tensor"])
    assert side * side == mesh.shape["tensor"] and mesh.shape["dp"] == 2
    finer = Mesh(
        mesh.devices.reshape(mesh.shape["pop"], mesh.shape["dp"], side, side),
        ("pop", "dp", "ty", "tx"),
    )
    placed = (
        P(("pop", "dp"), TENSOR),
        P("dp", TENSOR),
        P(("pop", "dp"), TENSOR, None),
        P(("pop", "dp"), None, TENSOR),
        P(("pop", "dp"), TENSOR),
        P("pop"),
        P(("pop", "dp")),
    )
    return jax.shard_map(
        functools.partial(local, side=side),
        mesh=finer,
        in_specs=placed,
        out_specs=(
            P(("pop", "dp"), TENSOR),
            P(("pop", "dp"), TENSOR),
            P(("pop", "dp"), TENSOR, None),
            P(("pop", "dp"), None, TENSOR),
        ),
        check_vma=False,
    )
```

```python
import functools
import math

import jax
import jax.numpy as jnp
from jax import lax
from jax.experimental import pallas as pl
from jax.experimental.pallas import tpu as pltpu
from jax.sharding import Mesh
from jax.sharding import PartitionSpec as P

MEMBERS = 4
BLOCK = 128
TENSOR = ("ty", "tx")
GROUP = ("dp", "ty", "tx")
EXTRA = 16
TOP = 32767.0


adapter_scale = 0.5


def ring_pairs(side, step, bulk):
    pairs = []
    for c in range(2):
        for y in range(side):
            for x in range(side):
                along_y = (c == 0) == bulk
                to_y = (y + step) % side if along_y else y
                to_x = x if along_y else (x + step) % side
                pairs.append(
                    ((c * side + y) * side + x, (c * side + to_y) * side + to_x)
                )
    return pairs


def send(x, side, step, bulk):
    return lax.ppermute(x, GROUP, ring_pairs(side, step, bulk))


def swap(x):
    return lax.ppermute(x, "dp", [(0, 1), (1, 0)])


def vmem(x):
    return pltpu.with_memory_space_constraint(x, pltpu.VMEM)


SCALARS = pl.BlockSpec(memory_space=pltpu.SMEM)
HBM = pl.BlockSpec(memory_space=pltpu.HBM)
ALL_VMEM = pl.BlockSpec(memory_space=pltpu.VMEM)
PARAMS = pltpu.CompilerParams(vmem_limit_bytes=10 << 20)


def pieces_kernel(x, out):
    n = out.shape[2]
    for j in range(out.shape[0]):
        out[j] = x[:, j * n : (j + 1) * n]


def in_pieces(weight, n, first, count):
    width = weight.shape[0]
    slabs = 4
    return pl.pallas_call(
        pieces_kernel,
        grid=(slabs,),
        out_shape=pltpu.HBM((count, width, n), weight.dtype),
        in_specs=[pl.BlockSpec((width // slabs, count * n), lambda i: (i, first // count))],
        out_specs=pl.BlockSpec((count, width // slabs, n), lambda i: (0, i, 0)),
        compiler_params=PARAMS,
        cost_estimate=pl.CostEstimate(
            flops=count * width * n, bytes_accessed=4 * count * width * n, transcendentals=0
        ),
    )(pltpu.with_memory_space_constraint(weight, pltpu.HBM))


def start_weight(pos, weights, buf, sem, slot, side, d, i):
    c, p, q = pos[0], pos[1], pos[2]
    chunk = lax.rem(p + (d + side), side)
    piece = lax.rem(q + (side - i), side)
    t = jnp.where(c == 0, side * chunk + piece, side * piece + chunk)
    count = weights[0].shape[0]
    parts = len(weights) // 2
    half = (t >= count * parts).astype(jnp.int32)
    row = t - half * (count * parts)
    part = lax.div(row, count)
    which = jnp.where(half == c, 0, parts) + part
    for k, ref in enumerate(weights):

        @pl.when(which == k)
        def _(ref=ref):
            pltpu.make_async_copy(ref.at[row - part * count], buf.at[slot], sem.at[slot]).start()


def wait_weight(weights, buf, sem, slot):
    pltpu.make_async_copy(weights[0].at[0], buf.at[slot], sem.at[slot]).wait()


def coded(acc):
    top = jnp.maximum(jnp.max(jnp.abs(acc), axis=0, keepdims=True), 1e-30)
    e = jnp.ceil(jnp.log2(top))
    q = jnp.round(acc * (jnp.exp2(-e) * TOP))
    q = jnp.clip(q, -TOP, TOP)
    return q.astype(jnp.int32).astype(jnp.int16), e


def scales(rows):
    return jnp.exp2(rows.astype(jnp.int32).astype(jnp.float32)) * (1.0 / TOP)


def reduce_kernel(pos, m, *refs, parts, side, d, first, count, arrived, last):
    refs = list(refs)
    weights = [refs.pop(0) for _ in range(parts)]
    recv = [refs.pop(0) for _ in arrived]
    if last:
        mine = refs.pop(0)
        outs = [refs.pop(0) for _ in range(count - 1)]
    else:
        out = refs.pop(0)
    wbuf, sem, es, *sin = refs
    n = m.shape[0]

    def begin(k, _):
        start_weight(pos, weights, wbuf, sem, k, side, d, first + k)
        return 0

    lax.fori_loop(0, count, begin, 0)
    for r, s, (_, held) in zip(recv, sin, arrived):
        s[...] = scales(r[held * n :, :])

    def piece(k, added):
        wait_weight(weights, wbuf, sem, k)
        acc = jnp.dot(m[...], wbuf[k], preferred_element_type=jnp.float32)
        for r, s, (start, _) in added:
            h = k + (first - start)
            at = pl.ds(pl.multiple_of(h * n, n), n)
            acc = acc + r[at, :].astype(jnp.int32).astype(jnp.float32) * s[pl.ds(h, 1), :]
        return acc

    sums = list(zip(recv, sin, arrived))
    if last:
        mine[...] = piece(0, sums)
        for k in range(1, count):
            q, e = coded(piece(k, sums))
            outs[k - 1][:n, :] = q
            outs[k - 1][n:, :] = (
                jnp.broadcast_to(e, (EXTRA, n)).astype(jnp.int32).astype(jnp.int16)
            )
        return

    es[...] = jnp.zeros_like(es)

    def body(k, _, added):
        q, e = coded(piece(k, added))
        out[pl.ds(pl.multiple_of(k * n, n), n), :] = q
        es[pl.ds(k, 1), :] = e
        return 0

    cuts = sorted({0, count, *(v for a, h in arrived for v in (a - first, a - first + h))})
    for lo, hi in zip(cuts, cuts[1:]):
        added = [t for t in sums if t[2][0] - first <= lo and hi <= t[2][0] - first + t[2][1]]
        lax.fori_loop(lo, hi, functools.partial(body, added=added), 0, unroll=2)
    out[count * n :, :] = es[...].astype(jnp.int32).astype(jnp.int16)


def reduce_step(pos, masked, weights, recv, arrived, side, d, first, count, last=False):
    tokens, width = masked.shape
    n = tokens
    if last:
        out_shape = [pltpu.VMEM((tokens, n), jnp.float32)] + [
            pltpu.VMEM((tokens + EXTRA, n), jnp.int16) for _ in range(count - 1)
        ]
    else:
        out_shape = pltpu.VMEM((count * tokens + EXTRA, n), jnp.int16)
    return pl.pallas_call(
        functools.partial(
            reduce_kernel,
            parts=len(weights),
            side=side,
            d=d,
            first=first,
            count=count,
            arrived=arrived,
            last=last,
        ),
        out_shape=out_shape,
        in_specs=[SCALARS, ALL_VMEM] + [HBM] * len(weights) + [ALL_VMEM] * len(recv),
        out_specs=[ALL_VMEM] * count if last else ALL_VMEM,
        scratch_shapes=[
            pltpu.VMEM((count, width, n), masked.dtype),
            pltpu.SemaphoreType.DMA((count,)),
        ]
        + [pltpu.VMEM((EXTRA, n), jnp.float32) for _ in range(1 + len(recv))],
        compiler_params=PARAMS,
        cost_estimate=pl.CostEstimate(
            flops=2 * tokens * n * width * count,
            bytes_accessed=count * n * (width + tokens * 2) * 2,
            transcendentals=0,
        ),
    )(pos, vmem(masked), *weights, *map(vmem, recv))


def gather_kernel(pos, acc, *refs, parts, side, held, last):
    refs = list(refs)
    weights = [refs.pop(0) for _ in range(parts)]
    chunks = [refs.pop(0) for _ in held]
    if last:
        extra, live = refs.pop(0), refs.pop(0)
    out, total, wbuf, sem = refs
    n = acc.shape[1]
    slots = []
    for d, first, count in held:
        at = slots[-1][1] if slots else 0
        slots.append((at, at + count))

        def begin(k, _, d=d, first=first, at=at):
            start_weight(pos, weights, wbuf, sem, at + k, side, d, first + k)
            return 0

        lax.fori_loop(0, count, begin, 0)
    total[...] = acc[...]
    for x, (at, end) in zip(chunks, slots):

        def body(k, _, x=x, at=at):
            wait_weight(weights, wbuf, sem, at + k)
            rows = x[pl.ds(pl.multiple_of(k * n, n), n), :]
            total[...] += lax.dot_general(
                wbuf[at + k],
                rows,
                (((1,), (1,)), ((), ())),
                preferred_element_type=jnp.float32,
            )
            return 0

        lax.fori_loop(0, end - at, body, 0, unroll=2)
    result = total[...]
    if last:
        result = live[...] * (result + adapter_scale * extra[...])
    out[...] = result.astype(out.dtype)


def gather_step(pos, acc, weights, chunks, held, side, extra=()):
    width, tokens = acc.shape
    count = sum(c for _, _, c in held)
    last = len(extra) > 0
    return pl.pallas_call(
        functools.partial(
            gather_kernel, parts=len(weights), side=side, held=held, last=last
        ),
        out_shape=pltpu.VMEM(acc.shape, jnp.bfloat16 if last else jnp.float32),
        in_specs=[SCALARS, ALL_VMEM]
        + [HBM] * len(weights)
        + [ALL_VMEM] * (len(chunks) + len(extra)),
        out_specs=ALL_VMEM,
        scratch_shapes=[
            pltpu.VMEM(acc.shape, jnp.float32),
            pltpu.VMEM((count, width, tokens), jnp.bfloat16),
            pltpu.SemaphoreType.DMA((count,)),
        ],
        compiler_params=PARAMS,
        cost_estimate=pl.CostEstimate(
            flops=2 * tokens * tokens * width * count,
            bytes_accessed=count * tokens * (width + tokens) * 2,
            transcendentals=0,
        ),
    )(pos, vmem(acc), *weights, *map(vmem, chunks), *map(vmem, extra))


def finish_kernel(mine, extra, *refs):
    *parts, out = refs
    n = mine.shape[0]
    total = mine[...] + adapter_scale * extra[...]
    for r in parts:
        s = scales(r[n:, :])[0:1, :]
        total = total + r[:n, :].astype(jnp.int32).astype(jnp.float32) * s
    out[...] = total.astype(out.dtype)


def finish(mine, extra, parts):
    return pl.pallas_call(
        finish_kernel,
        out_shape=jax.ShapeDtypeStruct(mine.shape, jnp.bfloat16),
        in_specs=[ALL_VMEM] * (2 + len(parts)),
        out_specs=ALL_VMEM,
        compiler_params=PARAMS,
    )(*map(vmem, (mine, extra, *parts)))


def block_members(member_blocks, first, count):
    ends = jnp.cumsum(member_blocks)
    blocks = first + jnp.arange(count, dtype=jnp.int32)
    return jnp.sum((ends[None, :] <= blocks[:, None]).astype(jnp.int32), axis=1)


def both_halves(x, c):
    other = swap(x)
    first = jnp.where(c == 0, x, other)
    second = jnp.where(c == 0, other, x)
    return jnp.concatenate([first, second], axis=0)


def exchange(x, side, bit, bulk):
    pairs = []
    for c in range(2):
        for y in range(side):
            for x_at in range(side):
                along_y = (c == 0) == bulk
                to_y, to_x = (y ^ bit, x_at) if along_y else (y, x_at ^ bit)
                pairs.append(
                    ((c * side + y) * side + x_at, (c * side + to_y) * side + to_x)
                )
    return lax.ppermute(x, GROUP, pairs)


def tie(*arrays):
    return lax.optimization_barrier(arrays)


def local(tokens, weight, adapter_in, adapter_out, cotangent, member_blocks, block_live, *, side):
    token_rows, width_local = tokens.shape
    hidden_local = weight.shape[1]
    blocks_here = token_rows // BLOCK
    c = lax.axis_index("dp").astype(jnp.int32)
    y = lax.axis_index("ty").astype(jnp.int32)
    x = lax.axis_index("tx").astype(jnp.int32)
    pos = jnp.stack([c, jnp.where(c == 0, y, x), jnp.where(c == 0, x, y)])
    far = side // 2

    parts = 2
    count = weight.shape[0] // width_local // parts
    own, whole, other = [], weight.T, []
    for k in range(parts):
        part = in_pieces(whole, width_local, k * count, count)
        part, whole, tokens, pos = tie(part, whole, tokens, pos)
        own.append(part)
        other.append(swap(part))
    weights = [pltpu.with_memory_space_constraint(w, pltpu.HBM) for w in own + other]

    shifts = [s if s <= far else s - side for s in range(side)]
    pieces = [tokens] + [send(tokens, side, s, False) for s in shifts[1:]]
    home = jnp.concatenate(pieces, axis=0)

    members = block_members(member_blocks, c * blocks_here, blocks_here)
    offsets = jnp.arange(BLOCK, dtype=jnp.int32)
    live = (offsets[None, :] < block_live[:, None]).astype(jnp.bfloat16).reshape(token_rows, 1)
    masked = cotangent * live

    down_all = both_halves(adapter_in, c)
    up_all = both_halves(adapter_out, c)
    chosen_in = jnp.take(down_all, members, axis=0)
    chosen_out = jnp.take(up_all, members, axis=0)
    token_blocks = tokens.reshape(blocks_here, BLOCK, width_local)
    grad_blocks = masked.reshape(blocks_here, BLOCK, hidden_local)
    part_in = jnp.einsum(
        "btk,bkr->btr", token_blocks, chosen_in, preferred_element_type=jnp.float32
    )
    part_back = jnp.einsum(
        "btf,brf->btr", grad_blocks, chosen_out, preferred_element_type=jnp.float32
    )
    rank = part_in.shape[-1]
    sums = jnp.concatenate([part_in, part_back], axis=-1).reshape(token_rows, 2 * rank)
    hops = [(1 << k, bulk) for bulk in (True, False) for k in range(side.bit_length() - 1)]

    def hop(sums, pos):
        sums, pos = tie(sums, pos)
        return sums, exchange(sums, side, *hops.pop(0)), pos

    def step(order, recv, arrived, **what):
        return reduce_step(order, masked, weights, recv, arrived, side, **what)

    def gather(order, total, chunks, held, extra=()):
        return gather_step(order, total, weights, chunks, held, side, extra)

    sums, moved, pos = hop(sums, pos)
    up, pos = tie(step(pos, [], (), d=far, first=0, count=far), pos)
    down, pos = tie(step(pos, [], (), d=-far, first=far, count=far), pos)
    up, down = send(up, side, 1, True), send(down, side, -1, True)
    ahead = send(home, side, 1, True)
    behind = send(home, side, -1, True)
    sums, moved, pos = hop(sums + moved, pos)
    total = jnp.zeros((hidden_local, token_rows), jnp.float32)
    total, pos = tie(gather(pos, total, [home], ((0, 0, side),)), pos)
    held_up, held_down = (0, far), (far, far)
    for k in range(1, far):
        if hops:
            sums, moved, pos = hop(sums + moved, pos)
        up = step(pos, [up], (held_up,), d=far - k, first=0, count=side)
        up, pos = tie(up, pos)
        up = send(up, side, 1, True)
        down = step(pos, [down], (held_down,), d=k - far, first=0, count=side)
        down, pos = tie(down, pos)
        down = send(down, side, -1, True)
        ahead, behind, pos = tie(ahead, behind, pos)
        held_up = held_down = (0, side)
        there, back = ahead, behind
        if k + 1 == far:
            ahead = ahead[: ahead.shape[0] // 2]
            behind = behind[behind.shape[0] // 2 :]
        ahead = send(ahead, side, 1, True)
        behind = send(behind, side, -1, True)
        if hops:
            sums, moved, pos = hop(sums + moved, pos)
        total = gather(pos, total, [there, back], ((-k, 0, side), (k, 0, side)))
        total, pos = tie(total, pos)
    sums, pos = tie((sums + moved).astype(jnp.bfloat16), pos)
    low_in = sums[:, :rank].reshape(blocks_here, BLOCK, rank)
    low_back = sums[:, rank:].reshape(blocks_here, BLOCK, rank)
    mine, *leaving = step(
        pos, [up, down], (held_up, held_down), d=0, first=0, count=side, last=True
    )
    *leaving, mine, pos = tie(*leaving, mine, pos)
    arrived = [send(a, side, -s, False) for a, s in zip(leaving, shifts[1:])]

    raised = jnp.einsum("btr,brf->fbt", low_in, chosen_out, preferred_element_type=jnp.float32)
    hidden = gather(
        pos,
        total,
        [ahead, behind],
        ((-far, 0, far), (far, far, far)),
        extra=(
            raised.reshape(hidden_local, token_rows),
            live.astype(jnp.float32).reshape(1, token_rows),
        ),
    ).T
    reduced = jnp.einsum("btr,bkr->btk", low_back, chosen_in, preferred_element_type=jnp.float32)
    input_gradient = finish(mine, reduced.reshape(token_rows, width_local), arrived)

    down_outer = jnp.einsum(
        "btk,btr->bkr", token_blocks, low_back, preferred_element_type=jnp.float32
    )
    up_outer = jnp.einsum("btr,btf->brf", low_in, grad_blocks, preferred_element_type=jnp.float32)

    def of_members(outer, first):
        owners = first + jnp.arange(MEMBERS // 2, dtype=jnp.int32)
        picked = (owners[:, None] == members[None, :])[:, :, None, None]
        return adapter_scale * jnp.where(picked, outer[None], 0.0).sum(axis=1)

    held_here = MEMBERS // 2
    down_grad = of_members(down_outer, c * held_here) + swap(
        of_members(down_outer, (1 - c) * held_here)
    )
    up_grad = of_members(up_outer, c * held_here) + swap(
        of_members(up_outer, (1 - c) * held_here)
    )
    return (hidden, input_gradient, down_grad, up_grad)


def solution(mesh):
    side = math.isqrt(mesh.shape["tensor"])
    assert side * side == mesh.shape["tensor"] and mesh.shape["dp"] == 2
    finer = Mesh(
        mesh.devices.reshape(mesh.shape["pop"], mesh.shape["dp"], side, side),
        ("pop", "dp", "ty", "tx"),
    )
    placed = (
        P(("pop", "dp"), TENSOR),
        P("dp", TENSOR),
        P(("pop", "dp"), TENSOR, None),
        P(("pop", "dp"), None, TENSOR),
        P(("pop", "dp"), TENSOR),
        P("pop"),
        P(("pop", "dp")),
    )

    def body(*args):
        return local(*args, side=side)

    return jax.shard_map(
        body,
        mesh=finer,
        in_specs=placed,
        out_specs=(
            P(("pop", "dp"), TENSOR),
            P(("pop", "dp"), TENSOR),
            P(("pop", "dp"), TENSOR, None),
            P(("pop", "dp"), None, TENSOR),
        ),
        check_vma=False,
    )
```

```python
import functools
import math

import jax
import jax.numpy as jnp
from jax import lax
from jax.experimental import pallas as pl
from jax.experimental.pallas import tpu as pltpu
from jax.sharding import Mesh
from jax.sharding import PartitionSpec as P

MEMBERS = 4
BLOCK = 128
TENSOR = ("ty", "tx")
GROUP = ("dp", "ty", "tx")
EXTRA = 16
TOP = 32767.0


adapter_scale = 0.5


def ring_pairs(side, step, bulk):
    pairs = []
    for c in range(2):
        for y in range(side):
            for x in range(side):
                along_y = (c == 0) == bulk
                to_y = (y + step) % side if along_y else y
                to_x = x if along_y else (x + step) % side
                pairs.append(
                    ((c * side + y) * side + x, (c * side + to_y) * side + to_x)
                )
    return pairs


def send(x, side, step, bulk):
    return lax.ppermute(x, GROUP, ring_pairs(side, step, bulk))


def swap(x):
    return lax.ppermute(x, "dp", [(0, 1), (1, 0)])


def vmem(x):
    return pltpu.with_memory_space_constraint(x, pltpu.VMEM)


HBM = pl.BlockSpec(memory_space=pltpu.HBM)
ALL_VMEM = pl.BlockSpec(memory_space=pltpu.VMEM)
PARAMS = pltpu.CompilerParams(vmem_limit_bytes=10 << 20)


def ring_place():
    c, y, x = (lax.axis_index(a).astype(jnp.int32) for a in GROUP)
    return c, jnp.where(c == 0, y, x), jnp.where(c == 0, x, y)


def start_weights(weights, buf, sem, side, wanted):
    own, other = weights
    n = buf.shape[2]
    here = own.shape[1] // n
    c, p, q = ring_place()
    for slot, (d, i) in enumerate(wanted):
        chunk = lax.rem(p + (d + side), side)
        piece = lax.rem(q + (side - i), side)
        t = jnp.where(c == 0, side * chunk + piece, side * piece + chunk)
        half = (t >= here).astype(jnp.int32)
        at = pl.ds(pl.multiple_of((t - half * here) * n, n), n)

        @pl.when(half == c)
        def _(at=at, slot=slot):
            pltpu.make_async_copy(own.at[:, at], buf.at[slot], sem.at[slot]).start()

        @pl.when(half != c)
        def _(at=at, slot=slot):
            pltpu.make_async_copy(other.at[:, at], buf.at[slot], sem.at[slot]).start()


def wait_weight(weights, buf, sem, slot):
    n = buf.shape[2]
    pltpu.make_async_copy(weights[0].at[:, pl.ds(0, n)], buf.at[slot], sem.at[slot]).wait()


def coded(acc):
    top = jnp.maximum(jnp.max(jnp.abs(acc), axis=0, keepdims=True), 1e-30)
    e = jnp.ceil(jnp.log2(top))
    q = jnp.round(acc * (jnp.exp2(-e) * TOP))
    q = jnp.clip(q, -TOP, TOP)
    return q.astype(jnp.int32).astype(jnp.int16), e


def scales(rows):
    return jnp.exp2(rows.astype(jnp.int32).astype(jnp.float32)) * (1.0 / TOP)


def reduce_kernel(m, *refs, parts, side, d, first, count, arrived, last):
    refs = list(refs)
    weights = [refs.pop(0) for _ in range(parts)]
    recv = [refs.pop(0) for _ in arrived]
    if last:
        mine = refs.pop(0)
        outs = [refs.pop(0) for _ in range(count - 1)]
    else:
        out = refs.pop(0)
    wbuf, sem, es, *sin = refs
    n = m.shape[0]

    start_weights(weights, wbuf, sem, side, [(d, first + k) for k in range(count)])
    for r, s, (_, held) in zip(recv, sin, arrived):
        s[...] = scales(r[held * n :, :])

    def piece(k, added):
        wait_weight(weights, wbuf, sem, k)
        acc = jnp.dot(m[...], wbuf[k], preferred_element_type=jnp.float32)
        for r, s, (start, _) in added:
            h = k + (first - start)
            at = pl.ds(pl.multiple_of(h * n, n), n)
            acc = acc + r[at, :].astype(jnp.int32).astype(jnp.float32) * s[pl.ds(h, 1), :]
        return acc

    sums = list(zip(recv, sin, arrived))
    if last:
        mine[...] = piece(0, sums)
        for k in range(1, count):
            q, e = coded(piece(k, sums))
            outs[k - 1][:n, :] = q
            outs[k - 1][n:, :] = (
                jnp.broadcast_to(e, (EXTRA, n)).astype(jnp.int32).astype(jnp.int16)
            )
        return

    es[...] = jnp.zeros_like(es)

    def body(k, _, added):
        q, e = coded(piece(k, added))
        out[pl.ds(pl.multiple_of(k * n, n), n), :] = q
        es[pl.ds(k, 1), :] = e
        return 0

    cuts = sorted({0, count, *(v for a, h in arrived for v in (a - first, a - first + h))})
    for lo, hi in zip(cuts, cuts[1:]):
        added = [t for t in sums if t[2][0] - first <= lo and hi <= t[2][0] - first + t[2][1]]
        lax.fori_loop(lo, hi, functools.partial(body, added=added), 0, unroll=4)
    out[count * n :, :] = es[...].astype(jnp.int32).astype(jnp.int16)


def reduce_step(masked, weights, recv, arrived, side, d, first, count, last=False):
    tokens, width = masked.shape
    n = tokens
    if last:
        out_shape = [pltpu.VMEM((tokens, n), jnp.float32)] + [
            pltpu.VMEM((tokens + EXTRA, n), jnp.int16) for _ in range(count - 1)
        ]
    else:
        out_shape = pltpu.VMEM((count * tokens + EXTRA, n), jnp.int16)
    return pl.pallas_call(
        functools.partial(
            reduce_kernel,
            parts=len(weights),
            side=side,
            d=d,
            first=first,
            count=count,
            arrived=arrived,
            last=last,
        ),
        out_shape=out_shape,
        in_specs=[ALL_VMEM] + [HBM] * len(weights) + [ALL_VMEM] * len(recv),
        out_specs=[ALL_VMEM] * count if last else ALL_VMEM,
        scratch_shapes=[
            pltpu.VMEM((count, width, n), masked.dtype),
            pltpu.SemaphoreType.DMA((count,)),
        ]
        + [pltpu.VMEM((EXTRA, n), jnp.float32) for _ in range(1 + len(recv))],
        compiler_params=PARAMS,
        cost_estimate=pl.CostEstimate(
            flops=2 * tokens * n * width * count,
            bytes_accessed=count * n * (width + tokens * 2) * 2,
            transcendentals=0,
        ),
    )(vmem(masked), *weights, *map(vmem, recv))


def gather_kernel(acc, *refs, parts, side, held, last):
    refs = list(refs)
    weights = [refs.pop(0) for _ in range(parts)]
    chunks = [refs.pop(0) for _ in held]
    if last:
        extra, live = refs.pop(0), refs.pop(0)
    out, total, wbuf, sem = refs
    n = acc.shape[1]
    start_weights(
        weights, wbuf, sem, side, [(d, first + k) for d, first, count in held for k in range(count)]
    )
    total[...] = acc[...]
    at = 0
    for x, (_, _, count) in zip(chunks, held):

        def body(k, _, x=x, at=at):
            wait_weight(weights, wbuf, sem, at + k)
            rows = x[pl.ds(pl.multiple_of(k * n, n), n), :]
            total[...] += lax.dot_general(
                wbuf[at + k], rows, (((1,), (1,)), ((), ())), preferred_element_type=jnp.float32
            )
            return 0

        lax.fori_loop(0, count, body, 0, unroll=4)
        at += count
    result = total[...]
    if last:
        result = live[...] * (result + adapter_scale * extra[...])
    out[...] = result.astype(out.dtype)


def gather_step(acc, weights, chunks, held, side, extra=()):
    width, tokens = acc.shape
    count = sum(c for _, _, c in held)
    last = len(extra) > 0
    return pl.pallas_call(
        functools.partial(
            gather_kernel, parts=len(weights), side=side, held=held, last=last
        ),
        out_shape=pltpu.VMEM(acc.shape, jnp.bfloat16 if last else jnp.float32),
        in_specs=[ALL_VMEM]
        + [HBM] * len(weights)
        + [ALL_VMEM] * (len(chunks) + len(extra)),
        out_specs=ALL_VMEM,
        scratch_shapes=[
            pltpu.VMEM(acc.shape, jnp.float32),
            pltpu.VMEM((count, width, tokens), jnp.bfloat16),
            pltpu.SemaphoreType.DMA((count,)),
        ],
        compiler_params=PARAMS,
        cost_estimate=pl.CostEstimate(
            flops=2 * tokens * tokens * width * count,
            bytes_accessed=count * tokens * (width + tokens) * 2,
            transcendentals=0,
        ),
    )(vmem(acc), *weights, *map(vmem, chunks), *map(vmem, extra))


def finish_kernel(mine, extra, *refs):
    *parts, out = refs
    n = mine.shape[0]
    total = mine[...] + adapter_scale * extra[...]
    for r in parts:
        s = scales(r[n:, :])[0:1, :]
        total = total + r[:n, :].astype(jnp.int32).astype(jnp.float32) * s
    out[...] = total.astype(out.dtype)


def finish(mine, extra, parts):
    return pl.pallas_call(
        finish_kernel,
        out_shape=jax.ShapeDtypeStruct(mine.shape, jnp.bfloat16),
        in_specs=[ALL_VMEM] * (2 + len(parts)),
        out_specs=ALL_VMEM,
        compiler_params=PARAMS,
    )(*map(vmem, (mine, extra, *parts)))


def block_members(member_blocks, first, count):
    ends = jnp.cumsum(member_blocks)
    blocks = first + jnp.arange(count, dtype=jnp.int32)
    return jnp.sum((ends[None, :] <= blocks[:, None]).astype(jnp.int32), axis=1)


def both_halves(x, c):
    other = swap(x)
    first = jnp.where(c == 0, x, other)
    second = jnp.where(c == 0, other, x)
    return jnp.concatenate([first, second], axis=0)


def exchange(x, side, bit, bulk):
    pairs = []
    for c in range(2):
        for y in range(side):
            for x_at in range(side):
                along_y = (c == 0) == bulk
                to_y, to_x = (y ^ bit, x_at) if along_y else (y, x_at ^ bit)
                pairs.append(
                    ((c * side + y) * side + x_at, (c * side + to_y) * side + to_x)
                )
    return lax.ppermute(x, GROUP, pairs)


def tie(*arrays):
    return lax.optimization_barrier(arrays)


def local(tokens, weight, adapter_in, adapter_out, cotangent, member_blocks, block_live, *, side):
    token_rows, width_local = tokens.shape
    hidden_local = weight.shape[1]
    blocks_here = token_rows // BLOCK
    c = lax.axis_index("dp").astype(jnp.int32)
    far = side // 2

    other = swap(weight.T)
    weights = [pltpu.with_memory_space_constraint(w, pltpu.HBM) for w in (weight.T, other)]

    shifts = [s if s <= far else s - side for s in range(side)]
    pieces = [tokens] + [send(tokens, side, s, False) for s in shifts[1:]]
    home = jnp.concatenate(pieces, axis=0)

    offsets = jnp.arange(BLOCK, dtype=jnp.int32)
    live = (offsets[None, :] < block_live[:, None]).astype(jnp.bfloat16).reshape(token_rows, 1)
    masked = cotangent * live

    def reduce(masked, recv, arrived, **what):
        return tie(reduce_step(masked, weights, recv, arrived, side, **what), masked)

    def gather(masked, total, chunks, held, extra=()):
        total, masked = tie(total, masked)
        return tie(gather_step(total, weights, chunks, held, side, extra), masked)

    up, masked = reduce(masked, [], (), d=far, first=0, count=far)
    down, masked = reduce(masked, [], (), d=-far, first=far, count=far)
    up, down = send(up, side, 1, True), send(down, side, -1, True)
    ahead = send(home, side, 1, True)
    behind = send(home, side, -1, True)

    adapter_in, adapter_out, masked = tie(adapter_in, adapter_out, masked)
    members = block_members(member_blocks, c * blocks_here, blocks_here)
    down_all = both_halves(adapter_in, c)
    up_all = both_halves(adapter_out, c)
    chosen_in = jnp.take(down_all, members, axis=0)
    chosen_out = jnp.take(up_all, members, axis=0)
    token_blocks = tokens.reshape(blocks_here, BLOCK, width_local)
    grad_blocks = masked.reshape(blocks_here, BLOCK, hidden_local)
    part_in = jnp.einsum(
        "btk,bkr->btr", token_blocks, chosen_in, preferred_element_type=jnp.float32
    )
    part_back = jnp.einsum(
        "btf,brf->btr", grad_blocks, chosen_out, preferred_element_type=jnp.float32
    )
    rank = part_in.shape[-1]
    sums = jnp.concatenate([part_in, part_back], axis=-1).reshape(token_rows, 2 * rank)
    bits = [1 << k for k in range(side.bit_length() - 1)]

    total = jnp.zeros((hidden_local, token_rows), jnp.float32)
    total, masked = gather(masked, total, [home], ((0, 0, side),))
    held_up, held_down = (0, far), (far, far)
    moved = None
    for k in range(1, far):
        if k <= len(bits):
            if moved is not None:
                sums, masked = tie(sums + moved, masked)
            moved = exchange(sums, side, bits[k - 1], True)
        up, masked = reduce(masked, [up], (held_up,), d=far - k, first=0, count=side)
        up = send(up, side, 1, True)
        down, masked = reduce(masked, [down], (held_down,), d=k - far, first=0, count=side)
        down = send(down, side, -1, True)
        held_up = held_down = (0, side)
        ahead, behind, masked = tie(ahead, behind, masked)
        there, back = ahead, behind
        if k + 1 == far:
            ahead = ahead[: ahead.shape[0] // 2]
            behind = behind[behind.shape[0] // 2 :]
        ahead = send(ahead, side, 1, True)
        behind = send(behind, side, -1, True)
        if k <= len(bits):
            sums, masked = tie(sums + moved, masked)
            moved = exchange(sums, side, bits[k - 1], False)
        total, masked = gather(masked, total, [there, back], ((-k, 0, side), (k, 0, side)))
    sums, masked = tie((sums + moved).astype(jnp.bfloat16), masked)
    low_in = sums[:, :rank].reshape(blocks_here, BLOCK, rank)
    low_back = sums[:, rank:].reshape(blocks_here, BLOCK, rank)
    mine, *leaving = reduce_step(
        masked,
        weights,
        [up, down],
        (held_up, held_down),
        side,
        d=0,
        first=0,
        count=side,
        last=True,
    )
    *leaving, mine, masked = tie(*leaving, mine, masked)
    arrived = [send(a, side, -s, False) for a, s in zip(leaving, shifts[1:])]

    raised = jnp.einsum("btr,brf->fbt", low_in, chosen_out, preferred_element_type=jnp.float32)
    hidden, masked = gather(
        masked,
        total,
        [ahead, behind],
        ((-far, 0, far), (far, far, far)),
        extra=(
            raised.reshape(hidden_local, token_rows),
            live.astype(jnp.float32).reshape(1, token_rows),
        ),
    )
    hidden = hidden.T
    reduced = jnp.einsum("btr,bkr->btk", low_back, chosen_in, preferred_element_type=jnp.float32)
    input_gradient = finish(mine, reduced.reshape(token_rows, width_local), arrived)

    down_outer = jnp.einsum(
        "btk,btr->bkr", token_blocks, low_back, preferred_element_type=jnp.float32
    )
    up_outer = jnp.einsum("btr,btf->brf", low_in, grad_blocks, preferred_element_type=jnp.float32)

    def of_members(outer, first):
        owners = first + jnp.arange(MEMBERS // 2, dtype=jnp.int32)
        picked = (owners[:, None] == members[None, :])[:, :, None, None]
        return adapter_scale * jnp.where(picked, outer[None], 0.0).sum(axis=1)

    held_here = MEMBERS // 2
    down_grad = of_members(down_outer, c * held_here) + swap(
        of_members(down_outer, (1 - c) * held_here)
    )
    up_grad = of_members(up_outer, c * held_here) + swap(
        of_members(up_outer, (1 - c) * held_here)
    )
    return (hidden, input_gradient, down_grad, up_grad)


def solution(mesh):
    side = math.isqrt(mesh.shape["tensor"])
    assert side * side == mesh.shape["tensor"] and mesh.shape["dp"] == 2
    finer = Mesh(
        mesh.devices.reshape(mesh.shape["pop"], mesh.shape["dp"], side, side),
        ("pop", "dp", "ty", "tx"),
    )
    placed = (
        P(("pop", "dp"), TENSOR),
        P("dp", TENSOR),
        P(("pop", "dp"), TENSOR, None),
        P(("pop", "dp"), None, TENSOR),
        P(("pop", "dp"), TENSOR),
        P("pop"),
        P(("pop", "dp")),
    )

    def body(*args):
        return local(*args, side=side)

    return jax.shard_map(
        body,
        mesh=finer,
        in_specs=placed,
        out_specs=(
            P(("pop", "dp"), TENSOR),
            P(("pop", "dp"), TENSOR),
            P(("pop", "dp"), TENSOR, None),
            P(("pop", "dp"), None, TENSOR),
        ),
        check_vma=False,
    )
```

```python
import functools
import math

import jax
import jax.numpy as jnp
from jax import lax
from jax.experimental import pallas as pl
from jax.experimental.pallas import tpu as pltpu
from jax.sharding import Mesh
from jax.sharding import PartitionSpec as P

MEMBERS = 4
BLOCK = 128
TENSOR = ("ty", "tx")
GROUP = ("dp", "ty", "tx")
EXTRA = 16
TOP = 32767.0


adapter_scale = 0.5


def ring_pairs(side, step, bulk):
    pairs = []
    for c in range(2):
        for y in range(side):
            for x in range(side):
                along_y = (c == 0) == bulk
                to_y = (y + step) % side if along_y else y
                to_x = x if along_y else (x + step) % side
                pairs.append(
                    ((c * side + y) * side + x, (c * side + to_y) * side + to_x)
                )
    return pairs


def send(x, side, step, bulk):
    return lax.ppermute(x, GROUP, ring_pairs(side, step, bulk))


def swap(x):
    return lax.ppermute(x, "dp", [(0, 1), (1, 0)])


def vmem(x):
    return pltpu.with_memory_space_constraint(x, pltpu.VMEM)


HBM = pl.BlockSpec(memory_space=pltpu.HBM)
ALL_VMEM = pl.BlockSpec(memory_space=pltpu.VMEM)
PARAMS = pltpu.CompilerParams(vmem_limit_bytes=10 << 20)


def ring_place():
    c, y, x = (lax.axis_index(a).astype(jnp.int32) for a in GROUP)
    return c, jnp.where(c == 0, y, x), jnp.where(c == 0, x, y)


def start_weights(weights, buf, sem, side, slot, d, first, count):
    own, other = weights
    n = buf.shape[2]
    here = own.shape[1] // n
    c, p, q = ring_place()
    chunk = lax.rem(p + (d + side), side)

    def begin(k, _):
        piece = lax.rem(q + (side - first) - k, side)
        t = jnp.where(c == 0, side * chunk + piece, side * piece + chunk)
        half = (t >= here).astype(jnp.int32)
        at = pl.ds(pl.multiple_of((t - half * here) * n, n), n)
        to = slot + k

        @pl.when(half == c)
        def _():
            pltpu.make_async_copy(own.at[:, at], buf.at[to], sem.at[to]).start()

        @pl.when(half != c)
        def _():
            pltpu.make_async_copy(other.at[:, at], buf.at[to], sem.at[to]).start()

        return 0

    lax.fori_loop(0, count, begin, 0)


def wait_weight(weights, buf, sem, slot):
    n = buf.shape[2]
    pltpu.make_async_copy(weights[0].at[:, pl.ds(0, n)], buf.at[slot], sem.at[slot]).wait()


def coded(acc):
    top = jnp.maximum(jnp.max(jnp.abs(acc), axis=0, keepdims=True), 1e-30)
    e = jnp.ceil(jnp.log2(top))
    q = jnp.round(acc * (jnp.exp2(-e) * TOP))
    q = jnp.clip(q, -TOP, TOP)
    return q.astype(jnp.int32).astype(jnp.int16), e


def scales(rows):
    return jnp.exp2(rows.astype(jnp.int32).astype(jnp.float32)) * (1.0 / TOP)


def reduce_kernel(m, *refs, parts, side, d, first, count, arrived, last):
    refs = list(refs)
    weights = [refs.pop(0) for _ in range(parts)]
    recv = [refs.pop(0) for _ in arrived]
    if last:
        mine = refs.pop(0)
        outs = [refs.pop(0) for _ in range(count - 1)]
    else:
        out = refs.pop(0)
    if last:
        held = refs.pop(0)
    wbuf, sem, es, *sin = refs
    n = m.shape[0]

    start_weights(weights, wbuf, sem, side, 0, d, first, count)
    for r, s, (_, rows) in zip(recv, sin, arrived):
        s[...] = scales(r[rows * n :, :])

    def piece(k, added):
        wait_weight(weights, wbuf, sem, k)
        acc = jnp.dot(m[...], wbuf[k], preferred_element_type=jnp.float32)
        for r, s, (start, _) in added:
            h = k + (first - start)
            at = pl.ds(pl.multiple_of(h * n, n), n)
            acc = acc + r[at, :].astype(jnp.int32).astype(jnp.float32) * s[pl.ds(h, 1), :]
        return acc

    sums = list(zip(recv, sin, arrived))
    if last:
        mine[...] = piece(0, sums)
        size = n + EXTRA

        def code(k, _):
            q, e = coded(piece(k, sums))
            at = pl.multiple_of((k - 1) * size, EXTRA)
            held[pl.ds(at, n), :] = q
            held[pl.ds(pl.multiple_of(at + n, EXTRA), EXTRA), :] = (
                jnp.broadcast_to(e, (EXTRA, n)).astype(jnp.int32).astype(jnp.int16)
            )
            return 0

        lax.fori_loop(1, count, code, 0)
        for k, out in enumerate(outs):
            out[...] = held[k * size : (k + 1) * size, :]
        return

    es[...] = jnp.zeros_like(es)

    def body(k, _, added):
        q, e = coded(piece(k, added))
        out[pl.ds(pl.multiple_of(k * n, n), n), :] = q
        es[pl.ds(k, 1), :] = e
        return 0

    cuts = sorted({0, count, *(v for a, h in arrived for v in (a - first, a - first + h))})
    for lo, hi in zip(cuts, cuts[1:]):
        added = [t for t in sums if t[2][0] - first <= lo and hi <= t[2][0] - first + t[2][1]]
        lax.fori_loop(lo, hi, functools.partial(body, added=added), 0, unroll=1 if len(cuts) > 2 else 2)
    out[count * n :, :] = es[...].astype(jnp.int32).astype(jnp.int16)


def reduce_step(masked, weights, recv, arrived, side, d, first, count, last=False):
    tokens, width = masked.shape
    n = tokens
    if last:
        out_shape = [pltpu.VMEM((tokens, n), jnp.float32)] + [
            pltpu.VMEM((tokens + EXTRA, n), jnp.int16) for _ in range(count - 1)
        ]
    else:
        out_shape = pltpu.VMEM((count * tokens + EXTRA, n), jnp.int16)
    return pl.pallas_call(
        functools.partial(
            reduce_kernel,
            parts=len(weights),
            side=side,
            d=d,
            first=first,
            count=count,
            arrived=arrived,
            last=last,
        ),
        out_shape=out_shape,
        in_specs=[ALL_VMEM] + [HBM] * len(weights) + [ALL_VMEM] * len(recv),
        out_specs=[ALL_VMEM] * count if last else ALL_VMEM,
        scratch_shapes=([pltpu.VMEM(((count - 1) * (n + EXTRA), n), jnp.int16)] if last else [])
        + [
            pltpu.VMEM((count, width, n), masked.dtype),
            pltpu.SemaphoreType.DMA((count,)),
        ]
        + [pltpu.VMEM((EXTRA, n), jnp.float32) for _ in range(1 + len(recv))],
        compiler_params=PARAMS,
        cost_estimate=pl.CostEstimate(
            flops=2 * tokens * n * width * count,
            bytes_accessed=count * n * (width + tokens * 2) * 2,
            transcendentals=0,
        ),
    )(vmem(masked), *weights, *map(vmem, recv))


def gather_kernel(acc, *refs, parts, side, held, last):
    refs = list(refs)
    weights = [refs.pop(0) for _ in range(parts)]
    chunks = [refs.pop(0) for _ in held]
    if last:
        extra, live = refs.pop(0), refs.pop(0)
    out, total, wbuf, sem = refs
    n = acc.shape[1]
    each = held[0][2]
    for h, (d, first, count) in enumerate(held):
        start_weights(weights, wbuf, sem, side, h * each, d, first, count)
    total[...] = acc[...]

    def body(k, _):
        at = pl.ds(pl.multiple_of(k * n, n), n)
        for h, x in enumerate(chunks):
            wait_weight(weights, wbuf, sem, h * each + k)
            total[...] += lax.dot_general(
                wbuf[h * each + k],
                x[at, :],
                (((1,), (1,)), ((), ())),
                preferred_element_type=jnp.float32,
            )
        return 0

    lax.fori_loop(0, each, body, 0, unroll=2 // len(held))
    result = total[...]
    if last:
        result = live[...] * (result + adapter_scale * extra[...])
    out[...] = result.astype(out.dtype)


def gather_step(acc, weights, chunks, held, side, extra=()):
    width, tokens = acc.shape
    count = sum(c for _, _, c in held)
    last = len(extra) > 0
    return pl.pallas_call(
        functools.partial(
            gather_kernel, parts=len(weights), side=side, held=held, last=last
        ),
        out_shape=pltpu.VMEM(acc.shape, jnp.bfloat16 if last else jnp.float32),
        in_specs=[ALL_VMEM]
        + [HBM] * len(weights)
        + [ALL_VMEM] * (len(chunks) + len(extra)),
        out_specs=ALL_VMEM,
        scratch_shapes=[
            pltpu.VMEM(acc.shape, jnp.float32),
            pltpu.VMEM((count, width, tokens), jnp.bfloat16),
            pltpu.SemaphoreType.DMA((count,)),
        ],
        compiler_params=PARAMS,
        cost_estimate=pl.CostEstimate(
            flops=2 * tokens * tokens * width * count,
            bytes_accessed=count * tokens * (width + tokens) * 2,
            transcendentals=0,
        ),
    )(vmem(acc), *weights, *map(vmem, chunks), *map(vmem, extra))


def finish_kernel(mine, extra, *refs):
    *parts, out = refs
    n = mine.shape[0]
    total = mine[...] + adapter_scale * extra[...]
    for r in parts:
        s = scales(r[n:, :])[0:1, :]
        total = total + r[:n, :].astype(jnp.int32).astype(jnp.float32) * s
    out[...] = total.astype(out.dtype)


def finish(mine, extra, parts):
    return pl.pallas_call(
        finish_kernel,
        out_shape=jax.ShapeDtypeStruct(mine.shape, jnp.bfloat16),
        in_specs=[ALL_VMEM] * (2 + len(parts)),
        out_specs=ALL_VMEM,
        compiler_params=PARAMS,
    )(*map(vmem, (mine, extra, *parts)))


def low_kernel(member_blocks, tokens, masked, own, other, sums, chosen):
    each, rank, _ = own.shape
    n = tokens.shape[1]
    blocks = chosen.shape[0]
    c = lax.axis_index("dp").astype(jnp.int32)
    for b in range(blocks):
        end, member = jnp.int32(0), jnp.int32(0)
        for m in range(2 * each - 1):
            end = end + member_blocks[m]
            member = member + (end <= c * blocks + b).astype(jnp.int32)
        half = (member >= each).astype(jnp.int32)
        at = member - half * each
        factors = jnp.where(half == c, own[at], other[at])
        chosen[b] = factors
        rows = slice(b * BLOCK, (b + 1) * BLOCK)
        for k, (x, f) in enumerate(((tokens, factors[:, :n]), (masked, factors[:, n:]))):
            sums[rows, k * rank : (k + 1) * rank] = lax.dot_general(
                x[rows, :], f, (((1,), (1,)), ((), ())), preferred_element_type=jnp.float32
            )


def low_parts(member_blocks, tokens, masked, own, other):
    blocks = tokens.shape[0] // BLOCK
    return pl.pallas_call(
        low_kernel,
        out_shape=[
            pltpu.VMEM((tokens.shape[0], 2 * own.shape[1]), jnp.float32),
            pltpu.VMEM((blocks, *own.shape[1:]), own.dtype),
        ],
        in_specs=[pl.BlockSpec(memory_space=pltpu.SMEM)] + [ALL_VMEM] * 4,
        out_specs=[ALL_VMEM] * 2,
        compiler_params=PARAMS,
        cost_estimate=pl.CostEstimate(
            flops=2 * tokens.shape[0] * own[0].size, bytes_accessed=4 * own.size, transcendentals=0
        ),
    )(member_blocks, *map(vmem, (tokens, masked, own, other)))


def block_members(member_blocks, first, count):
    ends = jnp.cumsum(member_blocks)
    blocks = first + jnp.arange(count, dtype=jnp.int32)
    return jnp.sum((ends[None, :] <= blocks[:, None]).astype(jnp.int32), axis=1)


def exchange(x, side, bit, bulk):
    pairs = []
    for c in range(2):
        for y in range(side):
            for x_at in range(side):
                along_y = (c == 0) == bulk
                to_y, to_x = (y ^ bit, x_at) if along_y else (y, x_at ^ bit)
                pairs.append(
                    ((c * side + y) * side + x_at, (c * side + to_y) * side + to_x)
                )
    return lax.ppermute(x, GROUP, pairs)


def tie(*arrays):
    return lax.optimization_barrier(arrays)


def local(tokens, weight, adapter_in, adapter_out, cotangent, member_blocks, block_live, *, side):
    token_rows, width_local = tokens.shape
    hidden_local = weight.shape[1]
    blocks_here = token_rows // BLOCK
    c = lax.axis_index("dp").astype(jnp.int32)
    far = side // 2

    other = swap(weight.T)
    weights = [pltpu.with_memory_space_constraint(w, pltpu.HBM) for w in (weight.T, other)]

    factors = jnp.concatenate([adapter_in.transpose(0, 2, 1), adapter_out], axis=2)
    other_factors = swap(factors)

    def near(x, step):
        return send(x, side, step, False)

    piece = {0: tokens, 1: near(tokens, 1), side - 1: near(tokens, -1)}
    offsets = jnp.arange(BLOCK, dtype=jnp.int32)
    live = (offsets[None, :] < block_live[:, None]).astype(jnp.bfloat16).reshape(token_rows, 1)
    masked = cotangent * live

    def reduce(masked, recv, arrived, **what):
        return tie(reduce_step(masked, weights, recv, arrived, side, **what), masked)

    def gather(masked, total, chunks, held, extra=()):
        total, masked = tie(total, masked)
        return tie(gather_step(total, weights, chunks, held, side, extra), masked)

    up, masked = reduce(masked, [], (), d=far, first=0, count=far)
    down, masked = reduce(masked, [], (), d=-far, first=far, count=far)
    up, down = send(up, side, 1, True), send(down, side, -1, True)
    below = jnp.concatenate([piece[0], piece[1]], axis=0)
    above = jnp.concatenate([piece[0], piece[side - 1]], axis=0)
    below, above = near(below, 2), near(above, -2)
    piece[2], piece[3] = below[:token_rows], below[token_rows:]
    piece[side - 2], piece[side - 3] = above[:token_rows], above[token_rows:]
    piece[4] = near(piece[3], 1)
    *pieces, masked = tie(*(piece[i] for i in range(side)), masked)
    home = jnp.concatenate(pieces, axis=0)
    ahead = send(home, side, 1, True)
    behind = send(home, side, -1, True)

    sums, chosen = low_parts(member_blocks, tokens, masked, factors, other_factors)
    sums, masked = tie(sums, masked)
    rank = factors.shape[1]
    chosen_in, chosen_out = chosen[:, :, :width_local], chosen[:, :, width_local:]
    token_blocks = tokens.reshape(blocks_here, BLOCK, width_local)
    grad_blocks = masked.reshape(blocks_here, BLOCK, hidden_local)
    bits = [1 << k for k in range(side.bit_length() - 1)]

    total = jnp.zeros((hidden_local, token_rows), jnp.float32)
    total, masked = gather(masked, total, [home], ((0, 0, side),))
    held_up, held_down = (0, far), (far, far)
    moved = None
    for k in range(1, far):
        if k <= len(bits):
            if moved is not None:
                sums, masked = tie(sums + moved, masked)
            moved = exchange(sums, side, bits[k - 1], True)
        up, masked = reduce(masked, [up], (held_up,), d=far - k, first=0, count=side)
        up = send(up, side, 1, True)
        down, masked = reduce(masked, [down], (held_down,), d=k - far, first=0, count=side)
        down = send(down, side, -1, True)
        held_up = held_down = (0, side)
        ahead, behind, masked = tie(ahead, behind, masked)
        there, back = ahead, behind
        if k + 1 == far:
            ahead = ahead[: ahead.shape[0] // 2]
            behind = behind[behind.shape[0] // 2 :]
        ahead = send(ahead, side, 1, True)
        behind = send(behind, side, -1, True)
        if k <= len(bits):
            sums, masked = tie(sums + moved, masked)
            moved = exchange(sums, side, bits[k - 1], False)
        total, masked = gather(masked, total, [there, back], ((-k, 0, side), (k, 0, side)))
    sums, masked = tie((sums + moved).astype(jnp.bfloat16), masked)
    low_in = sums[:, :rank].reshape(blocks_here, BLOCK, rank)
    low_back = sums[:, rank:].reshape(blocks_here, BLOCK, rank)
    mine, *leaving = reduce_step(
        masked,
        weights,
        [up, down],
        (held_up, held_down),
        side,
        d=0,
        first=0,
        count=side,
        last=True,
    )
    *leaving, mine, masked = tie(*leaving, mine, masked)
    arrived = [
        send(a, side, -s if s <= far else side - s, False)
        for s, a in enumerate(leaving, start=1)
    ]

    raised = jnp.einsum("btr,brf->fbt", low_in, chosen_out, preferred_element_type=jnp.float32)
    hidden, masked = gather(
        masked,
        total,
        [ahead, behind],
        ((-far, 0, far), (far, far, far)),
        extra=(
            raised.reshape(hidden_local, token_rows),
            live.astype(jnp.float32).reshape(1, token_rows),
        ),
    )
    hidden = hidden.T
    reduced = jnp.einsum("btr,brk->btk", low_back, chosen_in, preferred_element_type=jnp.float32)
    input_gradient = finish(mine, reduced.reshape(token_rows, width_local), arrived)

    down_outer = jnp.einsum(
        "btr,btk->brk", low_back, token_blocks, preferred_element_type=jnp.float32
    )
    up_outer = jnp.einsum("btr,btf->brf", low_in, grad_blocks, preferred_element_type=jnp.float32)
    outer = jnp.concatenate([down_outer, up_outer], axis=2)
    members = block_members(member_blocks, c * blocks_here, blocks_here)
    held_here = MEMBERS // 2

    def of_members(first):
        owners = first + jnp.arange(held_here, dtype=jnp.int32)
        picked = (owners[:, None] == members[None, :])[:, :, None, None]
        return adapter_scale * jnp.where(picked, outer[None], 0.0).sum(axis=1)

    grads = of_members(c * held_here) + swap(of_members((1 - c) * held_here))
    down_grad = grads[:, :, :width_local].transpose(0, 2, 1)
    return (hidden, input_gradient, down_grad, grads[:, :, width_local:])


def solution(mesh):
    side = math.isqrt(mesh.shape["tensor"])
    assert side == 8 and side * side == mesh.shape["tensor"] and mesh.shape["dp"] == 2
    finer = Mesh(
        mesh.devices.reshape(mesh.shape["pop"], mesh.shape["dp"], side, side),
        ("pop", "dp", "ty", "tx"),
    )
    placed = (
        P(("pop", "dp"), TENSOR),
        P("dp", TENSOR),
        P(("pop", "dp"), TENSOR, None),
        P(("pop", "dp"), None, TENSOR),
        P(("pop", "dp"), TENSOR),
        P("pop"),
        P(("pop", "dp")),
    )

    def body(*args):
        return local(*args, side=side)

    return jax.shard_map(
        body,
        mesh=finer,
        in_specs=placed,
        out_specs=(
            P(("pop", "dp"), TENSOR),
            P(("pop", "dp"), TENSOR),
            P(("pop", "dp"), TENSOR, None),
            P(("pop", "dp"), None, TENSOR),
        ),
        check_vma=False,
    )
```

```python
import functools
import math

import jax
import jax.numpy as jnp
from jax import lax
from jax.experimental import pallas as pl
from jax.experimental.pallas import tpu as pltpu
from jax.sharding import Mesh
from jax.sharding import PartitionSpec as P

BLOCK = 128
TENSOR = ("ty", "tx")
GROUP = ("dp", "ty", "tx")
EXTRA = 16
TOP = 32767.0


adapter_scale = 0.5


def ring_pairs(side, step, bulk):
    pairs = []
    for c in range(2):
        for y in range(side):
            for x in range(side):
                along_y = (c == 0) == bulk
                to_y = (y + step) % side if along_y else y
                to_x = x if along_y else (x + step) % side
                pairs.append(
                    ((c * side + y) * side + x, (c * side + to_y) * side + to_x)
                )
    return pairs


def send(x, side, step, bulk):
    return lax.ppermute(x, GROUP, ring_pairs(side, step, bulk))


def swap(x):
    return lax.ppermute(x, "dp", [(0, 1), (1, 0)])


def vmem(x):
    return pltpu.with_memory_space_constraint(x, pltpu.VMEM)


HBM = pl.BlockSpec(memory_space=pltpu.HBM)
ALL_VMEM = pl.BlockSpec(memory_space=pltpu.VMEM)
PARAMS = pltpu.CompilerParams(vmem_limit_bytes=10 << 20)


def ring_place():
    c, y, x = (lax.axis_index(a).astype(jnp.int32) for a in GROUP)
    return c, jnp.where(c == 0, y, x), jnp.where(c == 0, x, y)


def start_weights(weights, buf, sem, side, lane, d, first, count):
    own, other = weights
    n = buf.shape[2] // sem.shape[0]
    here = own.shape[1] // n
    c, p, q = ring_place()
    chunk = lax.rem(p + (d + side), side)

    def begin(k, _):
        piece = lax.rem(q + (side - first) - k, side)
        t = jnp.where(c == 0, side * chunk + piece, side * piece + chunk)
        half = (t >= here).astype(jnp.int32)
        at = pl.ds(pl.multiple_of((t - half * here) * n, n), n)
        to = buf.at[k, :, pl.ds(lane, n)]

        @pl.when(half == c)
        def _():
            pltpu.make_async_copy(own.at[:, at], to, sem.at[lane // n, k]).start()

        @pl.when(half != c)
        def _():
            pltpu.make_async_copy(other.at[:, at], to, sem.at[lane // n, k]).start()

        return 0

    lax.fori_loop(0, count, begin, 0)


def wait_weight(weights, buf, sem, slot):
    n = buf.shape[2] // sem.shape[0]
    for h in range(sem.shape[0]):
        pltpu.make_async_copy(
            weights[0].at[:, pl.ds(0, n)], buf.at[slot, :, pl.ds(h * n, n)], sem.at[h, slot]
        ).wait()


def coded(acc):
    top = jnp.maximum(jnp.max(jnp.abs(acc), axis=0, keepdims=True), 1e-30)
    e = jnp.ceil(jnp.log2(top))
    q = jnp.round(acc * (jnp.exp2(-e) * TOP))
    q = jnp.clip(q, -TOP, TOP)
    return q.astype(jnp.int32).astype(jnp.int16), e


def scales(rows):
    return jnp.exp2(rows.astype(jnp.int32).astype(jnp.float32)) * (1.0 / TOP)


def reduce_kernel(m, *refs, parts, side, d, first, count, arrived, last):
    refs = list(refs)
    weights = [refs.pop(0) for _ in range(parts)]
    recv = [refs.pop(0) for _ in arrived]
    if last:
        mine = refs.pop(0)
        outs = [refs.pop(0) for _ in range(count - 1)]
    else:
        out = refs.pop(0)
    if last:
        held = refs.pop(0)
    wbuf, sem, es, *sin = refs
    n = m.shape[0]

    start_weights(weights, wbuf, sem, side, 0, d, first, count)
    for r, s, (_, rows) in zip(recv, sin, arrived):
        s[...] = scales(r[rows * n :, :])

    def piece(k, added):
        wait_weight(weights, wbuf, sem, k)
        acc = jnp.dot(m[...], wbuf[k], preferred_element_type=jnp.float32)
        for r, s, (start, _) in added:
            h = k + (first - start)
            at = pl.ds(pl.multiple_of(h * n, n), n)
            acc = acc + r[at, :].astype(jnp.int32).astype(jnp.float32) * s[pl.ds(h, 1), :]
        return acc

    sums = list(zip(recv, sin, arrived))
    if last:
        mine[...] = piece(0, sums)
        size = n + EXTRA

        def code(k, _):
            q, e = coded(piece(k, sums))
            at = pl.multiple_of((k - 1) * size, EXTRA)
            held[pl.ds(at, n), :] = q
            held[pl.ds(pl.multiple_of(at + n, EXTRA), EXTRA), :] = (
                jnp.broadcast_to(e, (EXTRA, n)).astype(jnp.int32).astype(jnp.int16)
            )
            return 0

        lax.fori_loop(1, count, code, 0)
        for k, out in enumerate(outs):
            out[...] = held[k * size : (k + 1) * size, :]
        return

    es[...] = jnp.zeros_like(es)

    def body(k, _, added):
        q, e = coded(piece(k, added))
        out[pl.ds(pl.multiple_of(k * n, n), n), :] = q
        es[pl.ds(k, 1), :] = e
        return 0

    cuts = sorted({0, count, *(v for a, h in arrived for v in (a - first, a - first + h))})
    for lo, hi in zip(cuts, cuts[1:]):
        added = [t for t in sums if t[2][0] - first <= lo and hi <= t[2][0] - first + t[2][1]]
        lax.fori_loop(lo, hi, functools.partial(body, added=added), 0, unroll=1 if len(cuts) > 2 else 2)
    out[count * n :, :] = es[...].astype(jnp.int32).astype(jnp.int16)


def reduce_step(masked, weights, recv, arrived, side, d, first, count, last=False):
    tokens, width = masked.shape
    n = tokens
    if last:
        out_shape = [pltpu.VMEM((tokens, n), jnp.float32)] + [
            pltpu.VMEM((tokens + EXTRA, n), jnp.int16) for _ in range(count - 1)
        ]
    else:
        out_shape = pltpu.VMEM((count * tokens + EXTRA, n), jnp.int16)
    return pl.pallas_call(
        functools.partial(
            reduce_kernel,
            parts=len(weights),
            side=side,
            d=d,
            first=first,
            count=count,
            arrived=arrived,
            last=last,
        ),
        out_shape=out_shape,
        in_specs=[ALL_VMEM] + [HBM] * len(weights) + [ALL_VMEM] * len(recv),
        out_specs=[ALL_VMEM] * count if last else ALL_VMEM,
        scratch_shapes=([pltpu.VMEM(((count - 1) * (n + EXTRA), n), jnp.int16)] if last else [])
        + [
            pltpu.VMEM((count, width, n), masked.dtype),
            pltpu.SemaphoreType.DMA((1, count)),
        ]
        + [pltpu.VMEM((EXTRA, n), jnp.float32) for _ in range(1 + len(recv))],
        compiler_params=PARAMS,
        cost_estimate=pl.CostEstimate(
            flops=2 * tokens * n * width * count,
            bytes_accessed=count * n * (width + tokens * 2) * 2,
            transcendentals=0,
        ),
    )(vmem(masked), *weights, *map(vmem, recv))


def gather_kernel(acc, *refs, parts, side, held, last):
    refs = list(refs)
    weights = [refs.pop(0) for _ in range(parts)]
    chunks = [refs.pop(0) for _ in held]
    if last:
        extra, live = refs.pop(0), refs.pop(0)
    out, total, wbuf, sem = refs
    n = acc.shape[1]
    each = held[0][2]
    for h, (d, first, count) in enumerate(held):
        start_weights(weights, wbuf, sem, side, h * n, d, first, count)
    total[...] = acc[...]

    def body(k, _):
        at = pl.ds(pl.multiple_of(k * n, n), n)
        wait_weight(weights, wbuf, sem, k)
        rows = jnp.concatenate([x[at, :] for x in chunks], axis=1)
        total[...] += lax.dot_general(
            wbuf[k], rows, (((1,), (1,)), ((), ())), preferred_element_type=jnp.float32
        )
        return 0

    lax.fori_loop(0, each, body, 0, unroll=2)
    result = total[...]
    if last:
        result = live[...] * (result + adapter_scale * extra[...])
    out[...] = result.astype(out.dtype)


def gather_step(acc, weights, chunks, held, side, extra=()):
    width, tokens = acc.shape
    count = sum(c for _, _, c in held)
    last = len(extra) > 0
    return pl.pallas_call(
        functools.partial(
            gather_kernel, parts=len(weights), side=side, held=held, last=last
        ),
        out_shape=pltpu.VMEM(acc.shape, jnp.bfloat16 if last else jnp.float32),
        in_specs=[ALL_VMEM]
        + [HBM] * len(weights)
        + [ALL_VMEM] * (len(chunks) + len(extra)),
        out_specs=ALL_VMEM,
        scratch_shapes=[
            pltpu.VMEM(acc.shape, jnp.float32),
            pltpu.VMEM((count // len(held), width, tokens * len(held)), jnp.bfloat16),
            pltpu.SemaphoreType.DMA((len(held), count // len(held))),
        ],
        compiler_params=PARAMS,
        cost_estimate=pl.CostEstimate(
            flops=2 * tokens * tokens * width * count,
            bytes_accessed=count * tokens * (width + tokens) * 2,
            transcendentals=0,
        ),
    )(vmem(acc), *weights, *map(vmem, chunks), *map(vmem, extra))


def finish_kernel(mine, extra, *refs):
    *parts, out = refs
    n = mine.shape[0]
    total = mine[...] + adapter_scale * extra[...]
    for r in parts:
        s = scales(r[n:, :])[0:1, :]
        total = total + r[:n, :].astype(jnp.int32).astype(jnp.float32) * s
    out[...] = total.astype(out.dtype)


def finish(mine, extra, parts):
    return pl.pallas_call(
        finish_kernel,
        out_shape=jax.ShapeDtypeStruct(mine.shape, jnp.bfloat16),
        in_specs=[ALL_VMEM] * (2 + len(parts)),
        out_specs=ALL_VMEM,
        compiler_params=PARAMS,
    )(*map(vmem, (mine, extra, *parts)))


def low_kernel(member_blocks, tokens, masked, own, other, sums, chosen, table):
    each, rank, _ = own.shape
    n = tokens.shape[1]
    blocks = chosen.shape[0]
    c = lax.axis_index("dp").astype(jnp.int32)
    row = lax.broadcasted_iota(jnp.int32, table.shape, 0)
    lane = lax.broadcasted_iota(jnp.int32, table.shape, 1)
    asked = jnp.where(row < each, c * each + row, (1 - c) * each + (row - each))
    found = jnp.zeros(table.shape, jnp.float32)
    for b in range(blocks):
        end, member = jnp.int32(0), jnp.int32(0)
        for m in range(2 * each - 1):
            end = end + member_blocks[m]
            member = member + (end <= c * blocks + b).astype(jnp.int32)
        found = jnp.where((lane == b) & (asked == member), 1.0, found)
        half = (member >= each).astype(jnp.int32)
        at = member - half * each
        factors = jnp.where(half == c, own[at], other[at])
        chosen[b] = factors
        rows = slice(b * BLOCK, (b + 1) * BLOCK)
        for k, (x, f) in enumerate(((tokens, factors[:, :n]), (masked, factors[:, n:]))):
            sums[rows, k * rank : (k + 1) * rank] = lax.dot_general(
                x[rows, :], f, (((1,), (1,)), ((), ())), preferred_element_type=jnp.float32
            )
    table[...] = found


def low_parts(member_blocks, tokens, masked, own, other):
    blocks = tokens.shape[0] // BLOCK
    return pl.pallas_call(
        low_kernel,
        out_shape=[
            pltpu.VMEM((tokens.shape[0], 2 * own.shape[1]), jnp.float32),
            pltpu.VMEM((blocks, *own.shape[1:]), own.dtype),
            pltpu.VMEM((8, 128), jnp.float32),
        ],
        in_specs=[pl.BlockSpec(memory_space=pltpu.SMEM)] + [ALL_VMEM] * 4,
        out_specs=[ALL_VMEM] * 3,
        compiler_params=PARAMS,
        cost_estimate=pl.CostEstimate(
            flops=2 * tokens.shape[0] * own[0].size, bytes_accessed=4 * own.size, transcendentals=0
        ),
    )(member_blocks, *map(vmem, (tokens, masked, own, other)))


def exchange(x, side, bit, bulk):
    pairs = []
    for c in range(2):
        for y in range(side):
            for x_at in range(side):
                along_y = (c == 0) == bulk
                to_y, to_x = (y ^ bit, x_at) if along_y else (y, x_at ^ bit)
                pairs.append(
                    ((c * side + y) * side + x_at, (c * side + to_y) * side + to_x)
                )
    return lax.ppermute(x, GROUP, pairs)


def tie(*arrays):
    return lax.optimization_barrier(arrays)


def local(tokens, weight, adapter_in, adapter_out, cotangent, member_blocks, block_live, *, side):
    token_rows, width_local = tokens.shape
    hidden_local = weight.shape[1]
    blocks_here = token_rows // BLOCK
    far = side // 2

    other = swap(weight.T)
    weights = [pltpu.with_memory_space_constraint(w, pltpu.HBM) for w in (weight.T, other)]

    factors = jnp.concatenate([adapter_in.transpose(0, 2, 1), adapter_out], axis=2)
    other_factors = swap(factors)

    def near(x, step):
        return send(x, side, step, False)

    piece = {0: tokens, 1: near(tokens, 1), side - 1: near(tokens, -1)}
    offsets = jnp.arange(BLOCK, dtype=jnp.int32)
    live = (offsets[None, :] < block_live[:, None]).astype(jnp.bfloat16).reshape(token_rows, 1)
    masked = cotangent * live

    def reduce(masked, recv, arrived, **what):
        return tie(reduce_step(masked, weights, recv, arrived, side, **what), masked)

    def gather(masked, total, chunks, held, extra=()):
        total, masked = tie(total, masked)
        return tie(gather_step(total, weights, chunks, held, side, extra), masked)

    below = jnp.concatenate([piece[0], piece[1]], axis=0)
    above = jnp.concatenate([piece[0], piece[side - 1]], axis=0)
    below, above = near(below, 2), near(above, -2)
    up, masked = reduce(masked, [], (), d=far, first=0, count=far)
    below, above, masked = tie(below, above, masked)
    piece[2], piece[3] = below[:token_rows], below[token_rows:]
    piece[side - 2], piece[side - 3] = above[:token_rows], above[token_rows:]
    piece[4] = near(piece[3], 1)
    down, masked = reduce(masked, [], (), d=-far, first=far, count=far)
    up, down = send(up, side, 1, True), send(down, side, -1, True)
    *pieces, masked = tie(*(piece[i] for i in range(side)), masked)
    home = jnp.concatenate(pieces, axis=0)
    ahead = send(home, side, 1, True)
    behind = send(home, side, -1, True)

    sums, chosen, table = low_parts(member_blocks, tokens, masked, factors, other_factors)
    sums, masked = tie(sums, masked)
    rank = factors.shape[1]
    chosen_in, chosen_out = chosen[:, :, :width_local], chosen[:, :, width_local:]
    token_blocks = tokens.reshape(blocks_here, BLOCK, width_local)
    grad_blocks = masked.reshape(blocks_here, BLOCK, hidden_local)
    bits = [1 << k for k in range(side.bit_length() - 1)]

    total = jnp.zeros((hidden_local, token_rows), jnp.float32)
    total, masked = gather(masked, total, [home], ((0, 0, side),))
    held_up, held_down = (0, far), (far, far)
    moved = None
    for k in range(1, far):
        if k <= len(bits):
            if moved is not None:
                sums, masked = tie(sums + moved, masked)
            moved = exchange(sums, side, bits[k - 1], True)
        up, masked = reduce(masked, [up], (held_up,), d=far - k, first=0, count=side)
        up = send(up, side, 1, True)
        down, masked = reduce(masked, [down], (held_down,), d=k - far, first=0, count=side)
        down = send(down, side, -1, True)
        held_up = held_down = (0, side)
        ahead, behind, masked = tie(ahead, behind, masked)
        there, back = ahead, behind
        if k + 1 == far:
            ahead = ahead[: ahead.shape[0] // 2]
            behind = behind[behind.shape[0] // 2 :]
        ahead = send(ahead, side, 1, True)
        behind = send(behind, side, -1, True)
        if k <= len(bits):
            sums, masked = tie(sums + moved, masked)
            moved = exchange(sums, side, bits[k - 1], False)
        total, masked = gather(masked, total, [there, back], ((-k, 0, side), (k, 0, side)))
    sums, masked = tie((sums + moved).astype(jnp.bfloat16), masked)
    low_in = sums[:, :rank].reshape(blocks_here, BLOCK, rank)
    low_back = sums[:, rank:].reshape(blocks_here, BLOCK, rank)
    mine, *leaving = reduce_step(
        masked,
        weights,
        [up, down],
        (held_up, held_down),
        side,
        d=0,
        first=0,
        count=side,
        last=True,
    )
    *leaving, mine, masked = tie(*leaving, mine, masked)
    arrived = [
        send(a, side, -s if s <= far else side - s, False)
        for s, a in enumerate(leaving, start=1)
    ]

    raised = jnp.einsum("btr,brf->fbt", low_in, chosen_out, preferred_element_type=jnp.float32)
    hidden, masked = gather(
        masked,
        total,
        [ahead, behind],
        ((-far, 0, far), (far, far, far)),
        extra=(
            raised.reshape(hidden_local, token_rows),
            live.astype(jnp.float32).reshape(1, token_rows),
        ),
    )
    hidden = hidden.T
    reduced = jnp.einsum("btr,brk->btk", low_back, chosen_in, preferred_element_type=jnp.float32)
    input_gradient = finish(mine, reduced.reshape(token_rows, width_local), arrived)

    down_outer = jnp.einsum(
        "btr,btk->brk", low_back, token_blocks, preferred_element_type=jnp.float32
    )
    up_outer = jnp.einsum("btr,btf->brf", low_in, grad_blocks, preferred_element_type=jnp.float32)
    outer = jnp.concatenate([down_outer, up_outer], axis=2)
    each = adapter_in.shape[0]

    def of_members(first):
        share = table[first : first + each, :blocks_here, None, None]
        return adapter_scale * (share * outer[None]).sum(axis=1)

    grads = of_members(0) + swap(of_members(each))
    down_grad = grads[:, :, :width_local].transpose(0, 2, 1)
    return (hidden, input_gradient, down_grad, grads[:, :, width_local:])


def solution(mesh):
    side = math.isqrt(mesh.shape["tensor"])
    assert side == 8 and side * side == mesh.shape["tensor"] and mesh.shape["dp"] == 2
    finer = Mesh(
        mesh.devices.reshape(mesh.shape["pop"], mesh.shape["dp"], side, side),
        ("pop", "dp", "ty", "tx"),
    )
    placed = (
        P(("pop", "dp"), TENSOR),
        P("dp", TENSOR),
        P(("pop", "dp"), TENSOR, None),
        P(("pop", "dp"), None, TENSOR),
        P(("pop", "dp"), TENSOR),
        P("pop"),
        P(("pop", "dp")),
    )

    def body(*args):
        return local(*args, side=side)

    return jax.shard_map(
        body,
        mesh=finer,
        in_specs=placed,
        out_specs=(
            P(("pop", "dp"), TENSOR),
            P(("pop", "dp"), TENSOR),
            P(("pop", "dp"), TENSOR, None),
            P(("pop", "dp"), None, TENSOR),
        ),
        check_vma=False,
    )
```

```python
import functools
import math

import jax
import jax.numpy as jnp
from jax import lax
from jax.experimental import pallas as pl
from jax.experimental.pallas import tpu as pltpu
from jax.sharding import Mesh
from jax.sharding import PartitionSpec as P

BLOCK = 128
TENSOR = ("ty", "tx")
GROUP = ("dp", "ty", "tx")
EXTRA = 16
TOP = 32767.0


adapter_scale = 0.5


def ring_pairs(side, step, bulk):
    pairs = []
    for c in range(2):
        for y in range(side):
            for x in range(side):
                along_y = (c == 0) == bulk
                to_y = (y + step) % side if along_y else y
                to_x = x if along_y else (x + step) % side
                pairs.append(
                    ((c * side + y) * side + x, (c * side + to_y) * side + to_x)
                )
    return pairs


def send(x, side, step, bulk):
    return lax.ppermute(x, GROUP, ring_pairs(side, step, bulk))


def swap(x):
    return lax.ppermute(x, "dp", [(0, 1), (1, 0)])


def vmem(x):
    return pltpu.with_memory_space_constraint(x, pltpu.VMEM)


HBM = pl.BlockSpec(memory_space=pltpu.HBM)
ALL_VMEM = pl.BlockSpec(memory_space=pltpu.VMEM)
PARAMS = pltpu.CompilerParams(vmem_limit_bytes=10 << 20)


def ring_place():
    c, y, x = (lax.axis_index(a).astype(jnp.int32) for a in GROUP)
    return c, jnp.where(c == 0, y, x), jnp.where(c == 0, x, y)


def start_weights(weights, buf, sem, side, lane, d, first, count):
    own, other = weights
    n = buf.shape[2] // sem.shape[0]
    here = own.shape[1] // n
    c, p, q = ring_place()
    chunk = lax.rem(p + (d + side), side)

    def begin(k, _):
        piece = lax.rem(q + (side - first) - k, side)
        t = jnp.where(c == 0, side * chunk + piece, side * piece + chunk)
        half = (t >= here).astype(jnp.int32)
        at = pl.ds(pl.multiple_of((t - half * here) * n, n), n)
        to = buf.at[k, :, pl.ds(lane, n)]

        @pl.when(half == c)
        def _():
            pltpu.make_async_copy(own.at[:, at], to, sem.at[lane // n, k]).start()

        @pl.when(half != c)
        def _():
            pltpu.make_async_copy(other.at[:, at], to, sem.at[lane // n, k]).start()

        return 0

    lax.fori_loop(0, count, begin, 0)


def wait_weight(weights, buf, sem, slot):
    n = buf.shape[2] // sem.shape[0]
    for h in range(sem.shape[0]):
        pltpu.make_async_copy(
            weights[0].at[:, pl.ds(0, n)], buf.at[slot, :, pl.ds(h * n, n)], sem.at[h, slot]
        ).wait()


def coded(acc):
    top = jnp.maximum(jnp.max(jnp.abs(acc), axis=0, keepdims=True), 1e-30)
    e = jnp.ceil(jnp.log2(top))
    q = jnp.round(acc * (jnp.exp2(-e) * TOP))
    q = jnp.clip(q, -TOP, TOP)
    return q.astype(jnp.int32).astype(jnp.int16), e


def scales(rows):
    return jnp.exp2(rows.astype(jnp.int32).astype(jnp.float32)) * (1.0 / TOP)


def reduce_kernel(m, *refs, parts, side, d, first, count, arrived, last):
    refs = list(refs)
    weights = [refs.pop(0) for _ in range(parts)]
    recv = [refs.pop(0) for _ in arrived]
    if last:
        mine = refs.pop(0)
        outs = [refs.pop(0) for _ in range(count - 1)]
    else:
        out = refs.pop(0)
    if last:
        held = refs.pop(0)
    wbuf, sem, es, *sin = refs
    n = m.shape[0]

    start_weights(weights, wbuf, sem, side, 0, d, first, count)
    for r, s, (_, rows) in zip(recv, sin, arrived):
        s[...] = scales(r[rows * n :, :])

    def piece(k, added):
        wait_weight(weights, wbuf, sem, k)
        acc = jnp.dot(m[...], wbuf[k], preferred_element_type=jnp.float32)
        for r, s, (start, _) in added:
            h = k + (first - start)
            at = pl.ds(pl.multiple_of(h * n, n), n)
            acc = acc + r[at, :].astype(jnp.int32).astype(jnp.float32) * s[pl.ds(h, 1), :]
        return acc

    sums = list(zip(recv, sin, arrived))
    if last:
        mine[...] = piece(0, sums)
        size = n + EXTRA

        def code(k, _):
            q, e = coded(piece(k, sums))
            at = pl.multiple_of((k - 1) * size, EXTRA)
            held[pl.ds(at, n), :] = q
            held[pl.ds(pl.multiple_of(at + n, EXTRA), EXTRA), :] = (
                jnp.broadcast_to(e, (EXTRA, n)).astype(jnp.int32).astype(jnp.int16)
            )
            return 0

        lax.fori_loop(1, count, code, 0)
        for k, out in enumerate(outs):
            out[...] = held[k * size : (k + 1) * size, :]
        return

    es[...] = jnp.zeros_like(es)

    def body(k, _, added):
        q, e = coded(piece(k, added))
        out[pl.ds(pl.multiple_of(k * n, n), n), :] = q
        es[pl.ds(k, 1), :] = e
        return 0

    cuts = sorted({0, count, *(v for a, h in arrived for v in (a - first, a - first + h))})
    for lo, hi in zip(cuts, cuts[1:]):
        added = [t for t in sums if t[2][0] - first <= lo and hi <= t[2][0] - first + t[2][1]]
        lax.fori_loop(lo, hi, functools.partial(body, added=added), 0, unroll=1 if len(cuts) > 2 else 2)
    out[count * n :, :] = es[...].astype(jnp.int32).astype(jnp.int16)


def reduce_step(masked, weights, recv, arrived, side, d, first, count, last=False):
    tokens, width = masked.shape
    n = tokens
    if last:
        out_shape = [pltpu.VMEM((tokens, n), jnp.float32)] + [
            pltpu.VMEM((tokens + EXTRA, n), jnp.int16) for _ in range(count - 1)
        ]
    else:
        out_shape = pltpu.VMEM((count * tokens + EXTRA, n), jnp.int16)
    return pl.pallas_call(
        functools.partial(
            reduce_kernel,
            parts=len(weights),
            side=side,
            d=d,
            first=first,
            count=count,
            arrived=arrived,
            last=last,
        ),
        out_shape=out_shape,
        in_specs=[ALL_VMEM] + [HBM] * len(weights) + [ALL_VMEM] * len(recv),
        out_specs=[ALL_VMEM] * count if last else ALL_VMEM,
        scratch_shapes=([pltpu.VMEM(((count - 1) * (n + EXTRA), n), jnp.int16)] if last else [])
        + [
            pltpu.VMEM((count, width, n), masked.dtype),
            pltpu.SemaphoreType.DMA((1, count)),
        ]
        + [pltpu.VMEM((EXTRA, n), jnp.float32) for _ in range(1 + len(recv))],
        compiler_params=PARAMS,
        cost_estimate=pl.CostEstimate(
            flops=2 * tokens * n * width * count,
            bytes_accessed=count * n * (width + tokens * 2) * 2,
            transcendentals=0,
        ),
    )(vmem(masked), *weights, *map(vmem, recv))


def gather_kernel(acc, *refs, parts, side, held, last):
    refs = list(refs)
    weights = [refs.pop(0) for _ in range(parts)]
    chunks = [refs.pop(0) for _ in held]
    if last:
        extra, live = refs.pop(0), refs.pop(0)
    out, total, wbuf, sem = refs
    n = acc.shape[1]
    each = held[0][2]
    for h, (d, first, count) in enumerate(held):
        start_weights(weights, wbuf, sem, side, h * n, d, first, count)
    total[...] = acc[...]

    def body(k, _):
        at = pl.ds(pl.multiple_of(k * n, n), n)
        wait_weight(weights, wbuf, sem, k)
        rows = jnp.concatenate([x[at, :] for x in chunks], axis=1)
        total[...] += lax.dot_general(
            wbuf[k], rows, (((1,), (1,)), ((), ())), preferred_element_type=jnp.float32
        )
        return 0

    lax.fori_loop(0, each, body, 0, unroll=2)
    result = total[...]
    if last:
        result = live[...] * (result + adapter_scale * extra[...])
    out[...] = result.astype(out.dtype)


def gather_step(acc, weights, chunks, held, side, extra=()):
    width, tokens = acc.shape
    count = sum(c for _, _, c in held)
    last = len(extra) > 0
    return pl.pallas_call(
        functools.partial(
            gather_kernel, parts=len(weights), side=side, held=held, last=last
        ),
        out_shape=pltpu.VMEM(acc.shape, jnp.bfloat16 if last else jnp.float32),
        in_specs=[ALL_VMEM]
        + [HBM] * len(weights)
        + [ALL_VMEM] * (len(chunks) + len(extra)),
        out_specs=ALL_VMEM,
        scratch_shapes=[
            pltpu.VMEM(acc.shape, jnp.float32),
            pltpu.VMEM((count // len(held), width, tokens * len(held)), jnp.bfloat16),
            pltpu.SemaphoreType.DMA((len(held), count // len(held))),
        ],
        compiler_params=PARAMS,
        cost_estimate=pl.CostEstimate(
            flops=2 * tokens * tokens * width * count,
            bytes_accessed=count * tokens * (width + tokens) * 2,
            transcendentals=0,
        ),
    )(vmem(acc), *weights, *map(vmem, chunks), *map(vmem, extra))


def finish_kernel(mine, extra, *refs):
    *parts, out = refs
    n = mine.shape[0]
    total = mine[...] + adapter_scale * extra[...]
    for r in parts:
        s = scales(r[n:, :])[0:1, :]
        total = total + r[:n, :].astype(jnp.int32).astype(jnp.float32) * s
    out[...] = total.astype(out.dtype)


def finish(mine, extra, parts):
    return pl.pallas_call(
        finish_kernel,
        out_shape=jax.ShapeDtypeStruct(mine.shape, jnp.bfloat16),
        in_specs=[ALL_VMEM] * (2 + len(parts)),
        out_specs=ALL_VMEM,
        compiler_params=PARAMS,
    )(*map(vmem, (mine, extra, *parts)))


def low_kernel(member_blocks, tokens, masked, own, other, sums, chosen, table):
    each, rank, _ = own.shape
    n = tokens.shape[1]
    blocks = chosen.shape[0]
    c = lax.axis_index("dp").astype(jnp.int32)
    row = lax.broadcasted_iota(jnp.int32, table.shape, 0)
    lane = lax.broadcasted_iota(jnp.int32, table.shape, 1)
    asked = jnp.where(row < each, c * each + row, (1 - c) * each + (row - each))
    found = jnp.zeros(table.shape, jnp.float32)
    for b in range(blocks):
        end, member = jnp.int32(0), jnp.int32(0)
        for m in range(2 * each - 1):
            end = end + member_blocks[m]
            member = member + (end <= c * blocks + b).astype(jnp.int32)
        found = jnp.where((lane == b) & (asked == member), 1.0, found)
        half = (member >= each).astype(jnp.int32)
        at = member - half * each
        factors = jnp.where(half == c, own[at], other[at])
        chosen[b] = factors
        rows = slice(b * BLOCK, (b + 1) * BLOCK)
        for k, (x, f) in enumerate(((tokens, factors[:, :n]), (masked, factors[:, n:]))):
            sums[rows, k * rank : (k + 1) * rank] = lax.dot_general(
                x[rows, :], f, (((1,), (1,)), ((), ())), preferred_element_type=jnp.float32
            )
    table[...] = found


def low_parts(member_blocks, tokens, masked, own, other):
    blocks = tokens.shape[0] // BLOCK
    return pl.pallas_call(
        low_kernel,
        out_shape=[
            pltpu.VMEM((tokens.shape[0], 2 * own.shape[1]), jnp.float32),
            pltpu.VMEM((blocks, *own.shape[1:]), own.dtype),
            pltpu.VMEM((8, 128), jnp.float32),
        ],
        in_specs=[pl.BlockSpec(memory_space=pltpu.SMEM)] + [ALL_VMEM] * 4,
        out_specs=[ALL_VMEM] * 3,
        compiler_params=PARAMS,
        cost_estimate=pl.CostEstimate(
            flops=2 * tokens.shape[0] * own[0].size, bytes_accessed=4 * own.size, transcendentals=0
        ),
    )(member_blocks, *map(vmem, (tokens, masked, own, other)))


def exchange(x, side, bit, bulk):
    pairs = []
    for c in range(2):
        for y in range(side):
            for x_at in range(side):
                along_y = (c == 0) == bulk
                to_y, to_x = (y ^ bit, x_at) if along_y else (y, x_at ^ bit)
                pairs.append(
                    ((c * side + y) * side + x_at, (c * side + to_y) * side + to_x)
                )
    return lax.ppermute(x, GROUP, pairs)


def tie(*arrays):
    return lax.optimization_barrier(arrays)


def local(tokens, weight, adapter_in, adapter_out, cotangent, member_blocks, block_live, *, side):
    token_rows, width_local = tokens.shape
    hidden_local = weight.shape[1]
    blocks_here = token_rows // BLOCK
    far = side // 2

    other = swap(weight.T)
    weights = [pltpu.with_memory_space_constraint(w, pltpu.HBM) for w in (weight.T, other)]

    factors = jnp.concatenate([adapter_in.transpose(0, 2, 1), adapter_out], axis=2)
    other_factors = swap(factors)

    def near(x, step):
        return send(x, side, step, False)

    piece = {0: tokens, 1: near(tokens, 1), side - 1: near(tokens, -1)}
    offsets = jnp.arange(BLOCK, dtype=jnp.int32)
    live = (offsets[None, :] < block_live[:, None]).astype(jnp.bfloat16).reshape(token_rows, 1)
    masked = cotangent * live

    def reduce(masked, recv, arrived, **what):
        return tie(reduce_step(masked, weights, recv, arrived, side, **what), masked)

    def gather(masked, total, chunks, held, extra=()):
        total, masked = tie(total, masked)
        return tie(gather_step(total, weights, chunks, held, side, extra), masked)

    below = jnp.concatenate([piece[0], piece[1]], axis=0)
    above = jnp.concatenate([piece[0], piece[side - 1]], axis=0)
    below, above = near(below, 2), near(above, -2)
    up, masked = reduce(masked, [], (), d=far, first=0, count=far)
    below, above, masked = tie(below, above, masked)
    piece[2], piece[3] = below[:token_rows], below[token_rows:]
    piece[side - 2], piece[side - 3] = above[:token_rows], above[token_rows:]
    piece[4] = near(piece[3], 1)
    down, masked = reduce(masked, [], (), d=-far, first=far, count=far)
    up, down = send(up, side, 1, True), send(down, side, -1, True)
    *pieces, masked = tie(*(piece[i] for i in range(side)), masked)
    home = jnp.concatenate(pieces, axis=0)
    ahead = send(home, side, 1, True)
    behind = send(home, side, -1, True)

    sums, chosen, table = low_parts(member_blocks, tokens, masked, factors, other_factors)
    sums, masked = tie(sums, masked)
    rank = factors.shape[1]
    chosen_in, chosen_out = chosen[:, :, :width_local], chosen[:, :, width_local:]
    token_blocks = tokens.reshape(blocks_here, BLOCK, width_local)
    grad_blocks = masked.reshape(blocks_here, BLOCK, hidden_local)
    bits = [1 << k for k in range(side.bit_length() - 1)]

    total = jnp.zeros((hidden_local, token_rows), jnp.float32)
    total, masked = gather(masked, total, [home], ((0, 0, side),))
    held_up, held_down = (0, far), (far, far)
    moved = None
    for k in range(1, far):
        if k <= len(bits):
            if moved is not None:
                sums, masked = tie(sums + moved, masked)
            moved = exchange(sums, side, bits[k - 1], True)
        up, masked = reduce(masked, [up], (held_up,), d=far - k, first=0, count=side)
        up = send(up, side, 1, True)
        down, masked = reduce(masked, [down], (held_down,), d=k - far, first=0, count=side)
        down = send(down, side, -1, True)
        held_up = held_down = (0, side)
        ahead, behind, masked = tie(ahead, behind, masked)
        there, back = ahead, behind
        if k + 1 == far:
            ahead = ahead[: ahead.shape[0] // 2]
            behind = behind[behind.shape[0] // 2 :]
        ahead = send(ahead, side, 1, True)
        behind = send(behind, side, -1, True)
        if k <= len(bits):
            sums, masked = tie(sums + moved, masked)
            moved = exchange(sums, side, bits[k - 1], False)
        total, masked = gather(masked, total, [there, back], ((-k, 0, side), (k, 0, side)))
    sums, masked = tie((sums + moved).astype(jnp.bfloat16), masked)
    low_in = sums[:, :rank].reshape(blocks_here, BLOCK, rank)
    low_back = sums[:, rank:].reshape(blocks_here, BLOCK, rank)
    mine, *leaving = reduce_step(
        masked,
        weights,
        [up, down],
        (held_up, held_down),
        side,
        d=0,
        first=0,
        count=side,
        last=True,
    )
    *leaving, mine, masked = tie(*leaving, mine, masked)
    arrived = [
        send(a, side, -s if s <= far else side - s, False)
        for s, a in enumerate(leaving, start=1)
    ]

    raised = jnp.einsum("btr,brf->fbt", low_in, chosen_out, preferred_element_type=jnp.float32)
    hidden, masked = gather(
        masked,
        total,
        [ahead, behind],
        ((-far, 0, far), (far, far, far)),
        extra=(
            raised.reshape(hidden_local, token_rows),
            live.astype(jnp.float32).reshape(1, token_rows),
        ),
    )
    reduced = jnp.einsum("btr,brk->btk", low_back, chosen_in, preferred_element_type=jnp.float32)
    input_gradient = finish(mine, reduced.reshape(token_rows, width_local), arrived)

    down_outer = jnp.einsum(
        "btr,btk->brk", low_back, token_blocks, preferred_element_type=jnp.float32
    )
    up_outer = jnp.einsum("btr,btf->brf", low_in, grad_blocks, preferred_element_type=jnp.float32)
    outer = jnp.concatenate([down_outer, up_outer], axis=2)
    each = adapter_in.shape[0]

    def of_members(first):
        share = table[first : first + each, :blocks_here, None, None]
        return adapter_scale * (share * outer[None]).sum(axis=1)

    for_other, hidden = tie(of_members(each), hidden)
    grads = of_members(0) + swap(for_other)
    down_grad = grads[:, :, :width_local].transpose(0, 2, 1)
    return (hidden.T, input_gradient, down_grad, grads[:, :, width_local:])


def solution(mesh):
    side = math.isqrt(mesh.shape["tensor"])
    assert side == 8 and side * side == mesh.shape["tensor"] and mesh.shape["dp"] == 2
    finer = Mesh(
        mesh.devices.reshape(mesh.shape["pop"], mesh.shape["dp"], side, side),
        ("pop", "dp", "ty", "tx"),
    )
    placed = (
        P(("pop", "dp"), TENSOR),
        P("dp", TENSOR),
        P(("pop", "dp"), TENSOR, None),
        P(("pop", "dp"), None, TENSOR),
        P(("pop", "dp"), TENSOR),
        P("pop"),
        P(("pop", "dp")),
    )

    def body(*args):
        return local(*args, side=side)

    return jax.shard_map(
        body,
        mesh=finer,
        in_specs=placed,
        out_specs=(
            P(("pop", "dp"), TENSOR),
            P(("pop", "dp"), TENSOR),
            P(("pop", "dp"), TENSOR, None),
            P(("pop", "dp"), None, TENSOR),
        ),
        check_vma=False,
    )
```
